32 devices in a mesh: rep: 1 (over z), dp: 32 (over x, y, core).
Axes of the slice: x: 4, y: 4, z: 1, core: 2. Of those that a mesh axis runs over, the one named last changes fastest.
The devices are a block of a 4x4x8 slice.
Arguments:
- x: bfloat16 [32, 2048, 768], P(('rep', 'dp'))
- dy: bfloat16 [32, 2048, 768], P(('rep', 'dp'))
- wq: bfloat16 [2, 768, 768], replicated
- wk: bfloat16 [2, 768, 128], replicated
- wv: bfloat16 [2, 768, 128], replicated
- wo: bfloat16 [2, 768, 768], replicated
- w_gate: bfloat16 [2, 768, 2048], replicated
- w_up: bfloat16 [2, 768, 2048], replicated
- w_down: bfloat16 [2, 2048, 768], replicated
- m_wq: float32 [2, 768, 768], P(None, 'dp')
- m_wk: float32 [2, 768, 128], P(None, 'dp')
- m_wv: float32 [2, 768, 128], P(None, 'dp')
- m_wo: float32 [2, 768, 768], P(None, 'dp')
- m_w_gate: float32 [2, 768, 2048], P(None, 'dp')
- m_w_up: float32 [2, 768, 2048], P(None, 'dp')
- m_w_down: float32 [2, 2048, 768], P(None, 'dp')
- v_wq: float32 [2, 768, 768], P(None, 'dp')
- v_wk: float32 [2, 768, 128], P(None, 'dp')
- v_wv: float32 [2, 768, 128], P(None, 'dp')
- v_wo: float32 [2, 768, 768], P(None, 'dp')
- v_w_gate: float32 [2, 768, 2048], P(None, 'dp')
- v_w_up: float32 [2, 768, 2048], P(None, 'dp')
- v_w_down: float32 [2, 2048, 768], P(None, 'dp')
Outputs:
- output 1: bfloat16 [2, 768, 768], P('rep')
- output 2: bfloat16 [2, 768, 128], P('rep')
- output 3: bfloat16 [2, 768, 128], P('rep')
- output 4: bfloat16 [2, 768, 768], P('rep')
- output 5: bfloat16 [2, 768, 2048], P('rep')
- output 6: bfloat16 [2, 768, 2048], P('rep')
- output 7: bfloat16 [2, 2048, 768], P('rep')
- output 8: float32 [2, 768, 768], P('rep', 'dp')
- output 9: float32 [2, 768, 128], P('rep', 'dp')
- output 10: float32 [2, 768, 128], P('rep', 'dp')
- output 11: float32 [2, 768, 768], P('rep', 'dp')
- output 12: float32 [2, 768, 2048], P('rep', 'dp')
- output 13: float32 [2, 768, 2048], P('rep', 'dp')
- output 14: float32 [2, 2048, 768], P('rep', 'dp')
- output 15: float32 [2, 768, 768], P('rep', 'dp')
- output 16: float32 [2, 768, 128], P('rep', 'dp')
- output 17: float32 [2, 768, 128], P('rep', 'dp')
- output 18: float32 [2, 768, 768], P('rep', 'dp')
- output 19: float32 [2, 768, 2048], P('rep', 'dp')
- output 20: float32 [2, 768, 2048], P('rep', 'dp')
- output 21: float32 [2, 2048, 768], P('rep', 'dp')
All inputs are finite; a program needn't handle non-finite values.
Results may differ from the reference program's by a relative error of at most 0.0326.
Values are sent between devices in bfloat16 or wider.
A program may use at most 768 MiB of HBM per device.

```python
import jax
import jax.numpy as jnp
from jax import lax

SEQUENCES = 32
TOKENS = 2048
D = 768
HEADS = 6
KV_HEADS = 1
HEAD = 128
FF = 2048
LAYERS = 2
THETA = 10000
NAMES = ("wq", "wk", "wv", "wo", "w_gate", "w_up", "w_down")
SHAPES = {
    "wq": (LAYERS, D, HEADS * HEAD),
    "wk": (LAYERS, D, KV_HEADS * HEAD),
    "wv": (LAYERS, D, KV_HEADS * HEAD),
    "wo": (LAYERS, HEADS * HEAD, D),
    "w_gate": (LAYERS, D, FF),
    "w_up": (LAYERS, D, FF),
    "w_down": (LAYERS, FF, D),
}


def bump(key, n, height):
    away = (jnp.arange(n, dtype=jnp.int32) - jax.random.randint(key, (), 0, n, jnp.int32)) % n
    return jnp.where(away < n // 8, height, 1.0)


def together(key, own, strength):
    shared = jax.random.normal(key, own.shape[1:], jnp.float32)
    return (own + strength * shared) * lax.rsqrt(1 + strength * strength)


def setup_inputs(seed: int = 0, part: int = 0) -> dict:
    kx, kdy, ka, kb, kz, kf, kh, kl, *keys = jax.random.split(jax.random.key(seed), 8 + 3 * len(NAMES))
    kx, kdy, ka, kb = (jax.random.fold_in(k, part) for k in (kx, kdy, ka, kb))
    kw, km, kv = (keys[i::3] for i in range(3))
    shape = (SEQUENCES, TOKENS, D)
    much_x, much_dy = jax.random.uniform(kz, (2,), jnp.float32, 0.0, 1.0)
    loud = 2.0 ** jax.random.uniform(jax.random.fold_in(kz, 1), (), jnp.float32, -1.0, 2.0)
    layers = 2.0 ** jax.random.uniform(kl, (LAYERS, 1, 1), jnp.float32, -1.0, 1.0)
    times = {"wq": 1.0, "wk": 1.0, "wv": 2.0, "wo": layers, "w_gate": 1.0, "w_up": bump(kh, FF, 4.0), "w_down": layers}
    x = together(ka, jax.random.normal(kx, shape, jnp.float32), much_x) * bump(kf, D, 4.0)
    dy = together(kb, jax.random.normal(kdy, shape, jnp.float32), much_dy)
    drawn = {"x": x.astype(jnp.bfloat16), "dy": (loud * dy * (SEQUENCES * TOKENS) ** -0.5).astype(jnp.bfloat16)}
    for key, name in zip(kw, NAMES, strict=True):
        drawn[name] = (jax.random.normal(key, SHAPES[name], jnp.float32) * SHAPES[name][1] ** -0.5 * times[name]).astype(jnp.bfloat16)
    for key, name in zip(km, NAMES, strict=True):
        drawn[f"m_{name}"] = 0.1 * jax.random.normal(key, SHAPES[name], jnp.float32)
    for key, name in zip(kv, NAMES, strict=True):
        drawn[f"v_{name}"] = jax.random.uniform(key, SHAPES[name], jnp.float32, 0.02, 0.06)
    return drawn


def matmul(a, w):
    return jnp.dot(a, w, preferred_element_type=jnp.float32).astype(jnp.bfloat16)


def normed(h):
    wide = h.astype(jnp.float32)
    scale = lax.rsqrt(jnp.mean(wide**2, -1, keepdims=True) + 1e-6)
    return (wide * scale).astype(jnp.bfloat16)


def turned(t, theta):
    half = t.shape[-1] // 2
    angle = jnp.arange(t.shape[0], dtype=jnp.float32)[:, None] * theta ** (-jnp.arange(half, dtype=jnp.float32) / half)
    cos, sin = jnp.cos(angle)[:, None], jnp.sin(angle)[:, None]
    a, b = t[..., :half].astype(jnp.float32), t[..., half:].astype(jnp.float32)
    return jnp.concatenate([a * cos - b * sin, b * cos + a * sin], -1).astype(jnp.bfloat16)


def seen_by(q, k, v):
    tokens, kv = q.shape[0], k.shape[1]
    q = q.reshape(tokens, kv, -1, q.shape[-1])
    scores = jnp.einsum("tgsd,ugd->gstu", q.astype(jnp.float32), k.astype(jnp.float32)) * q.shape[-1] ** -0.5
    place = jnp.arange(tokens)
    weights = jax.nn.softmax(jnp.where(place[:, None] >= place, scores, -jnp.inf), -1).astype(jnp.bfloat16)
    return jnp.einsum("gstu,ugd->tgsd", weights.astype(jnp.float32), v.astype(jnp.float32)).astype(jnp.bfloat16).reshape(tokens, -1)


def layer(h, w):
    a = normed(h)
    q, k = (turned(matmul(a, w[name]).reshape(h.shape[0], -1, HEAD), THETA) for name in ("wq", "wk"))
    h = h + matmul(seen_by(q, k, matmul(a, w["wv"]).reshape(h.shape[0], -1, HEAD)), w["wo"])
    b = normed(h)
    gate = jnp.dot(b, w["w_gate"], preferred_element_type=jnp.float32)
    up = jnp.dot(b, w["w_up"], preferred_element_type=jnp.float32)
    return h + matmul((jax.nn.silu(gate) * up).astype(jnp.bfloat16), w["w_down"])


def adamw(w, m, v, g):
    m = 0.9 * m + 0.1 * g
    v = 0.95 * v + 0.05 * g * g
    step = m * lax.rsqrt(v + 1e-8) + 0.1 * w
    return (w - 0.02 * step).astype(jnp.bfloat16), m, v


def clipped(gradients, sum_of_squares, count):
    factor = jnp.minimum(1.0, 0.5 * lax.rsqrt(sum_of_squares / count + 1e-30))
    return [g * factor for g in gradients]


def stack(weights, h):
    return lax.scan(lambda h, w: (layer(h, w), None), h, weights)[0]


def reference(x, dy, wq, wk, wv, wo, w_gate, w_up, w_down, m_wq, m_wk, m_wv, m_wo, m_w_gate, m_w_up, m_w_down, v_wq, v_wk, v_wv, v_wo, v_w_gate, v_w_up, v_w_down):
    weights = dict(zip(NAMES, (wq, wk, wv, wo, w_gate, w_up, w_down), strict=True))

    def take(so_far, sequence):
        h, by_y = sequence
        _, back = jax.vjp(stack, weights, h)
        by_weights, by_h = back(by_y)
        return jax.tree.map(lambda total, term: total + term.astype(jnp.float32), so_far, by_weights), by_h

    none_yet = {name: jnp.zeros(w.shape, jnp.float32) for name, w in weights.items()}
    by_weights, by_x = lax.scan(take, none_yet, (x, dy))
    gradients = [by_weights[name].astype(jnp.bfloat16).astype(jnp.float32) for name in NAMES]
    gradients = clipped(gradients, sum(jnp.sum(g * g) for g in gradients), sum(g.size for g in gradients))
    first = (m_wq, m_wk, m_wv, m_wo, m_w_gate, m_w_up, m_w_down)
    second = (v_wq, v_wk, v_wv, v_wo, v_w_gate, v_w_up, v_w_down)
    new = [adamw(weights[name].astype(jnp.float32), m, v, g) for name, m, v, g in zip(NAMES, first, second, gradients, strict=True)]
    return tuple(one[which] for which in range(3) for one in new)
```

```python
import functools
import math

import jax
import jax.numpy as jnp
from jax import lax
from jax.experimental import pallas as pl
from jax.experimental.pallas import tpu as pltpu
from jax.sharding import PartitionSpec as P

HEAD = 128
THETA = 10000
NAMES = ("wq", "wk", "wv", "wo", "w_gate", "w_up", "w_down")
NEG = -1e30
LOG2E = 1.4426950408889634
VMEM = 56 * 2**20
MOST = 63 * 2**20


def dot(a, b, ca=1, cb=0):
    return lax.dot_general(a, b, (((ca,), (cb,)), ((), ())), preferred_element_type=jnp.float32)


def low(a):
    return a.astype(jnp.bfloat16)


def wide(a):
    return a.astype(jnp.float32)


def root(h):
    return lax.rsqrt(jnp.mean(h * h, -1, keepdims=True) + 1e-6)


def norm_back(h, r, by_a):
    return r * (by_a - h * (r * r * jnp.mean(h * by_a, -1, keepdims=True)))


def turned(t, cos, sin, way=1):
    other = pltpu.roll(t, HEAD // 2, 1) * sin
    return t * cos + other if way > 0 else t * cos - other


def heads_of(width):
    return [slice(at, at + HEAD) for at in range(0, width, HEAD)]


def project(a, wq, w_kv, cos, sin, q_ref, k_ref, v_ref):
    q, kv = low(dot(a, wq)), low(dot(a, w_kv))
    for at in heads_of(q.shape[1]):
        q_ref[:, at] = low(turned(wide(q[:, at]), cos, sin))
    k_ref[:] = low(turned(wide(kv[:, :HEAD]), cos, sin))
    v_ref[:] = kv[:, HEAD:]


def _pre(h_ref, cos_ref, sin_ref, wq_ref, wk_ref, wv_ref, q_ref, k_ref, v_ref, w_kv):
    @pl.when(pl.program_id(0) == 0)
    def _():
        w_kv[:, :HEAD] = wk_ref[0]
        w_kv[:, HEAD:] = wv_ref[0]

    h = wide(h_ref[:])
    project(low(h * root(h)), wq_ref[0], w_kv[:], cos_ref[:], sin_ref[:], q_ref, k_ref, v_ref)


def rows(bt, width, last=None):
    return pl.BlockSpec((bt, width), lambda i: (i if last is None else jnp.minimum(i, last), 0))


def one_layer(w, number):
    return pl.BlockSpec((1, *w.shape[1:]), lambda i: (number, 0, 0), pipeline_mode=pl.Buffered(1))


def like(rows, cols, dtype=jnp.bfloat16):
    return jax.ShapeDtypeStruct((rows, cols), dtype)


def params():
    return pltpu.CompilerParams(dimension_semantics=("arbitrary",), vmem_limit_bytes=MOST)


def cost(flops, arrays):
    return pl.CostEstimate(flops=int(flops), transcendentals=0, bytes_accessed=sum(a.size * a.dtype.itemsize for a in arrays))


def pre(h, tables, w, number, bt=512):
    tokens, d = h.shape
    wq, wk, wv = (w[name] for name in NAMES[:3])
    dk = wk.shape[2]
    return pl.pallas_call(
        _pre,
        grid=(tokens // bt,),
        in_specs=[rows(bt, d)] + [rows(bt, HEAD)] * 2 + [one_layer(a, number) for a in (wq, wk, wv)],
        out_specs=[rows(bt, wq.shape[2]), rows(bt, dk), rows(bt, dk)],
        out_shape=[like(tokens, wq.shape[2]), like(tokens, dk), like(tokens, dk)],
        scratch_shapes=[pltpu.VMEM((d, 2 * dk), jnp.bfloat16)],
        compiler_params=params(),
        cost_estimate=cost(2 * tokens * d * (wq.shape[2] + 2 * dk), (h, wq)),
        name="pre",
    )(h, *tables, wq, wk, wv)


def gated(gate, up):
    return gate * jax.nn.sigmoid(gate) * up


def _mid(h_ref, o_ref, cos_ref, sin_ref, wo_ref, wg_ref, wu_ref, wd_ref, wq_ref, wk_ref, wv_ref,
         h2_ref, gate_ref, up_ref, h3_ref, q_ref, k_ref, v_ref, w_kv, s_s, *, cut):
    @pl.when(pl.program_id(0) == 0)
    def _():
        w_kv[:, :HEAD] = wk_ref[0]
        w_kv[:, HEAD:] = wv_ref[0]

    h2 = low(wide(h_ref[:]) + wide(low(dot(o_ref[:], wo_ref[0]))))
    h2_ref[:] = h2
    h = wide(h2)
    b = low(h * root(h))
    for f in range(0, wg_ref.shape[2], cut):
        at = slice(f, f + cut)
        gate, up = dot(b, wg_ref[0, :, at]), dot(b, wu_ref[0, :, at])
        gate_ref[:, at] = gate
        up_ref[:, at] = up
        s_s[:, at] = low(gated(gate, up))
    h3 = low(h + wide(low(dot(s_s[:], wd_ref[0]))))
    h3_ref[:] = h3
    h = wide(h3)
    project(low(h * root(h)), wq_ref[0], w_kv[:], cos_ref[:], sin_ref[:], q_ref, k_ref, v_ref)


def mid(h, o, tables, w, number, bt=256, cut=512):
    tokens, d = h.shape
    wq, wk, wv, wo, wg, wu, wd = (w[name] for name in NAMES)
    dk, ff = wk.shape[2], wg.shape[2]
    return pl.pallas_call(
        functools.partial(_mid, cut=cut),
        grid=(tokens // bt,),
        in_specs=[rows(bt, d), rows(bt, d)] + [rows(bt, HEAD)] * 2 + [one_layer(a, number) for a in (wo, wg, wu, wd)]
        + [one_layer(a, number + 1) for a in (wq, wk, wv)],
        out_specs=[rows(bt, d), rows(bt, ff), rows(bt, ff), rows(bt, d), rows(bt, wq.shape[2]), rows(bt, dk), rows(bt, dk)],
        out_shape=[like(tokens, d), like(tokens, ff, jnp.float32), like(tokens, ff, jnp.float32), like(tokens, d),
                   like(tokens, wq.shape[2]), like(tokens, dk), like(tokens, dk)],
        scratch_shapes=[pltpu.VMEM((d, 2 * dk), jnp.bfloat16), pltpu.VMEM((bt, ff), jnp.bfloat16)],
        compiler_params=params(),
        cost_estimate=cost(2 * tokens * d * (d + 3 * ff + wq.shape[2] + 2 * dk), (h, wq)),
        name="mid",
    )(h, o, *tables, wo, wg, wu, wd, wq, wk, wv)


def _tail(h_ref, o_ref, dy_ref, *rest, blocks, cut, out, saved):
    if saved:
        gate_ref, up_ref, *rest = rest
    (wo_ref, wg_ref, wu_ref, wd_ref, dh2_ref, do_ref, delta_ref, gg_ref, gu_ref, gd_ref, go_ref,
     b_t, dy_t, s_s, dgate_s, dup_s, go_s) = rest
    i = pl.program_id(0)
    bt, d = dy_ref.shape
    ff = wg_ref.shape[2]

    @pl.when(i == 0)
    def _():
        go_s[:] = jnp.zeros_like(go_s)

    @pl.when(i < blocks)
    def _():
        here = pl.ds(pl.multiple_of(i * bt, bt), bt)
        o, dy = o_ref[:], dy_ref[:]
        h = wide(h_ref[:]) if saved else wide(low(wide(h_ref[:]) + wide(low(dot(o, wo_ref[0])))))
        r = root(h)
        b = low(h * r)
        by_b = jnp.zeros((bt, d), jnp.float32)
        for f in range(0, ff, cut):
            at = slice(f, f + cut)
            if saved:
                gate, up = gate_ref[:, at], up_ref[:, at]
            else:
                gate, up = dot(b, wg_ref[0, :, at]), dot(b, wu_ref[0, :, at])
            by_s = dot(dy, wd_ref[0, at, :], 1, 1)
            sig = jax.nn.sigmoid(gate)
            act = gate * sig
            s_s[here, at] = low(act * up)
            dup = low(by_s * act)
            dgate = low(by_s * up * (sig + act * (1 - sig)))
            dup_s[here, at] = dup
            dgate_s[here, at] = dgate
            by_b += dot(dgate, wg_ref[0, :, at], 1, 1) + dot(dup, wu_ref[0, :, at], 1, 1)
        dh2 = low(wide(dy) + norm_back(h, r, by_b))
        dh2_ref[:] = dh2
        do = low(dot(dh2, wo_ref[0], 1, 1))
        do_ref[:] = do
        both = wide(do) * wide(o)
        first = low(both)
        second = low(both - wide(first))
        own = lax.broadcasted_iota(jnp.int32, (8, d), 1) // HEAD == lax.broadcasted_iota(jnp.int32, (8, d), 0)
        pick = jnp.where(own, 1.0, 0.0).astype(jnp.bfloat16)
        delta_ref[:] = dot(pick, first, 1, 1) + dot(pick, second, 1, 1)
        b_t[:, here] = b.T
        dy_t[:, here] = dy.T
        got = dot(o.T, dh2)
        go_s[:] += got

    @pl.when(i >= blocks)
    def _():
        at = pl.ds(pl.multiple_of((i - blocks) * out, out), out)
        gg_ref[:] = low(dot(b_t[:], dgate_s[:, at]))
        gu_ref[:] = low(dot(b_t[:], dup_s[:, at]))
        gd_ref[:] = low(dot(dy_t[:], s_s[:, at]).T)

    @pl.when(i == pl.num_programs(0) - 1)
    def _():
        go_ref[:] = low(go_s[:])


def tail(h, o, dy, w, number, kept=None, bt=256, cut=512, out=256):
    tokens, d = dy.shape
    wo, wg, wu, wd = (w[name] for name in NAMES[3:])
    ff = wg.shape[2]
    blocks, last = tokens // bt, tokens // bt - 1
    after = lambda i: jnp.maximum(i - blocks, 0)
    whole = lambda a, b: pl.BlockSpec((a, b), lambda i: (0, 0), pipeline_mode=pl.Buffered(1))
    return pl.pallas_call(
        functools.partial(_tail, blocks=blocks, cut=cut, out=out, saved=kept is not None),
        grid=(blocks + ff // out,),
        in_specs=[rows(bt, d, last)] * 3 + ([] if kept is None else [rows(bt, ff, last)] * 2) + [one_layer(a, number) for a in (wo, wg, wu, wd)],
        out_specs=[rows(bt, d, last), rows(bt, d, last), pl.BlockSpec((8, bt), lambda i: (0, jnp.minimum(i, last))),
                   pl.BlockSpec((d, out), lambda i: (0, after(i))), pl.BlockSpec((d, out), lambda i: (0, after(i))),
                   pl.BlockSpec((out, d), lambda i: (after(i), 0)), whole(d, d)],
        out_shape=[like(tokens, d), like(tokens, d), like(8, tokens, jnp.float32), like(d, ff), like(d, ff), like(ff, d), like(d, d)],
        scratch_shapes=[pltpu.VMEM((d, tokens), jnp.bfloat16)] * 2 + [pltpu.VMEM((tokens, ff), jnp.bfloat16)] * 3 + [pltpu.VMEM((d, d), jnp.float32)],
        compiler_params=params(),
        cost_estimate=cost(2 * tokens * d * (3 * d + 8 * ff), (h, o, dy)),
        name="tail",
    )(h, o, dy, *(kept or ()), wo, wg, wu, wd)


def _back(h_ref, dh2_ref, dq_ref, dk_ref, dv_ref, cos_ref, sin_ref, wq_ref, wk_ref, wv_ref, *rest, blocks, first):
    dh_ref, rest = (None, rest) if first else (rest[0], rest[1:])
    gq_ref, gk_ref, gv_ref, a_t, d_s = rest
    i = pl.program_id(0)
    bt, d = h_ref.shape
    dq_w = dq_ref.shape[1]
    here = pl.ds(pl.multiple_of(i * bt, bt), bt)
    h = wide(h_ref[:])
    r = root(h)
    a_t[:, here] = low(h * r).T
    cos, sin = cos_ref[:], sin_ref[:]
    for at in heads_of(dq_w):
        d_s[here, at] = low(turned(wide(dq_ref[:, at]), cos, sin, -1))
    d_s[here, dq_w : dq_w + HEAD] = low(turned(wide(dk_ref[:]), cos, sin, -1))
    d_s[here, dq_w + HEAD :] = dv_ref[:]
    if not first:
        mine = d_s[here, :]
        by_a = dot(mine[:, :dq_w], wq_ref[0], 1, 1)
        by_a += dot(mine[:, dq_w : dq_w + HEAD], wk_ref[0], 1, 1) + dot(mine[:, dq_w + HEAD :], wv_ref[0], 1, 1)
        dh_ref[:] = low(wide(dh2_ref[:]) + norm_back(h, r, by_a))

    @pl.when(i == blocks - 1)
    def _():
        got = low(dot(a_t[:], d_s[:]))
        gq_ref[:] = got[:, :dq_w]
        gk_ref[:] = got[:, dq_w : dq_w + HEAD]
        gv_ref[:] = got[:, dq_w + HEAD :]


def back(h, dh2, dq, dk, dv, tables, w, number, bt=512):
    tokens, d = h.shape
    wq, wk, wv = (w[name] for name in NAMES[:3])
    first = number == 0
    blocks = tokens // bt
    whole = lambda a: pl.BlockSpec(a.shape[1:], lambda i: (0, 0))
    return pl.pallas_call(
        functools.partial(_back, blocks=blocks, first=first),
        grid=(blocks,),
        in_specs=[rows(bt, d), rows(bt, d), rows(bt, dq.shape[1]), rows(bt, HEAD), rows(bt, HEAD), rows(bt, HEAD), rows(bt, HEAD)]
        + [one_layer(a, number) for a in (wq, wk, wv)],
        out_specs=([] if first else [rows(bt, d)]) + [whole(a) for a in (wq, wk, wv)],
        out_shape=([] if first else [like(tokens, d)]) + [like(*a.shape[1:]) for a in (wq, wk, wv)],
        scratch_shapes=[pltpu.VMEM((d, tokens), jnp.bfloat16), pltpu.VMEM((tokens, dq.shape[1] + 2 * HEAD), jnp.bfloat16)],
        compiler_params=params(),
        cost_estimate=cost(4 * tokens * d * (d + 2 * HEAD), (h, dq)),
        name="back",
    )(h, dh2, dq, dk, dv, *tables, wq, wk, wv)


def tables_of(tokens):
    half = HEAD // 2
    angle = jnp.arange(tokens, dtype=jnp.float32)[:, None] * THETA ** (-jnp.arange(half, dtype=jnp.float32) / half)
    cos, sin = jnp.cos(angle), jnp.sin(angle)
    return jnp.concatenate([cos, cos], 1), jnp.concatenate([-sin, sin], 1)


def cut_off(bk, bq, first_key, first_query):
    return lax.broadcasted_iota(jnp.int32, (bk, bq), 1) + first_query >= lax.broadcasted_iota(jnp.int32, (bk, bq), 0) + first_key


def _forward(q_ref, k_ref, v_ref, o_ref, lse_ref, top_s, mix_s, *, bq, bk, scale):
    heads = heads_of(q_ref.shape[1])
    iq = pl.program_id(0)
    e = scale * LOG2E
    top_s[:] = jnp.full(top_s.shape, NEG, jnp.float32)
    mix_s[:] = jnp.zeros_like(mix_s)
    ones = jnp.ones((8, bk), jnp.bfloat16)

    def block(j, masked):
        here = pl.ds(pl.multiple_of(j * bk, bk), bk)
        k = k_ref[here, :]
        values = jnp.concatenate([v_ref[here, :].T, ones], axis=0)
        scores = [dot(k, q_ref[:, at], 1, 1) for at in heads]
        ok = cut_off(bk, bq, j * bk, iq * bq) if masked else None
        weights, keeps = [], []
        for n, s in enumerate(scores):
            if masked:
                s = jnp.where(ok, s, 2 * NEG)
            old = top_s[n : n + 1, :]
            top = jnp.maximum(old, s.max(axis=0, keepdims=True))
            top_s[n : n + 1, :] = top
            weights.append(low(jnp.exp2((s - top) * e)))
            keeps.append(jnp.exp2((old - top) * e))
        for n, (p, keep) in enumerate(zip(weights, keeps)):
            mix_s[n] = mix_s[n] * keep + dot(values, p)

    whole = lax.div(iq * bq, bk)
    lax.fori_loop(0, whole, lambda j, _: block(j, False), None)
    for j in range(bq // bk):
        block(whole + j, True)
    for n, at in enumerate(heads):
        total = mix_s[n, HEAD : HEAD + 1, :]
        o_ref[:, at] = low((mix_s[n, :HEAD, :] * (1 / total)).T)
        lse_ref[n : n + 1, :] = top_s[n : n + 1, :] * scale + jnp.log(total)


def attend(q, k, v, bq=512, bk=512):
    tokens, width = q.shape
    heads = width // HEAD
    whole = pl.BlockSpec((tokens, HEAD), lambda i: (0, 0))
    return pl.pallas_call(
        functools.partial(_forward, bq=bq, bk=bk, scale=HEAD**-0.5),
        grid=(tokens // bq,),
        in_specs=[rows(bq, width), whole, whole],
        out_specs=[rows(bq, width), pl.BlockSpec((8, bq), lambda i: (0, i))],
        out_shape=[like(tokens, width), like(8, tokens, jnp.float32)],
        scratch_shapes=[pltpu.VMEM((8, bq), jnp.float32), pltpu.VMEM((heads, HEAD + 8, bq), jnp.float32)],
        compiler_params=params(),
        cost_estimate=cost(2 * tokens * tokens * width, (q, q, k, v)),
        name="attend",
    )(q, k, v)


def _backward(q_ref, k_ref, v_ref, do_ref, lse_ref, delta_ref, dq_ref, dk_ref, dv_ref, dq_s, dk_s, dv_s, *, bq, bk, scale):
    heads = heads_of(q_ref.shape[1])
    iq = pl.program_id(0)
    e = scale * LOG2E

    @pl.when(iq == 0)
    def _():
        dk_s[:] = jnp.zeros_like(dk_s)
        dv_s[:] = jnp.zeros_like(dv_s)

    dq_s[:] = jnp.zeros_like(dq_s)

    def block(j, masked):
        here = pl.ds(pl.multiple_of(j * bk, bk), bk)
        k, v = k_ref[here, :], v_ref[here, :]
        k_t = k.T
        ok = cut_off(bk, bq, j * bk, iq * bq) if masked else None
        scores = [dot(k, q_ref[:, at], 1, 1) for at in heads]
        dps = [dot(v, do_ref[:, at], 1, 1) for at in heads]
        for n, at in enumerate(heads):
            p = jnp.exp2(scores[n] * e - lse_ref[n : n + 1, :] * LOG2E)
            if masked:
                p = jnp.where(ok, p, 0.0)
            ds = low(p * (dps[n] - delta_ref[n : n + 1, :]))
            dv_s[here, :] += dot(low(p), do_ref[:, at])
            dk_s[here, :] += dot(ds, q_ref[:, at])
            dq_s[n] += dot(k_t, ds)

    whole = lax.div(iq * bq, bk)
    lax.fori_loop(0, whole, lambda j, _: block(j, False), None)
    for j in range(bq // bk):
        block(whole + j, True)
    for n, at in enumerate(heads):
        dq_ref[:, at] = low((dq_s[n] * scale).T)

    @pl.when(iq == pl.num_programs(0) - 1)
    def _():
        dk_ref[:] = low(dk_s[:] * scale)
        dv_ref[:] = low(dv_s[:])


def attend_back(q, k, v, do, lse, delta, bq=512, bk=512):
    tokens, width = q.shape
    heads = width // HEAD
    whole = pl.BlockSpec((tokens, HEAD), lambda i: (0, 0))
    stats = pl.BlockSpec((8, bq), lambda i: (0, i))
    return pl.pallas_call(
        functools.partial(_backward, bq=bq, bk=bk, scale=HEAD**-0.5),
        grid=(tokens // bq,),
        in_specs=[rows(bq, width), whole, whole, rows(bq, width), stats, stats],
        out_specs=[rows(bq, width), whole, whole],
        out_shape=[like(tokens, width), like(tokens, HEAD), like(tokens, HEAD)],
        scratch_shapes=[pltpu.VMEM((heads, HEAD, bq), jnp.float32), pltpu.VMEM((tokens, HEAD), jnp.float32), pltpu.VMEM((tokens, HEAD), jnp.float32)],
        compiler_params=params(),
        cost_estimate=cost(5 * tokens * tokens * width, (q, q, q, k, v)),
        name="attend_back",
    )(q, k, v, do, lse, delta)


CORES = 2


class Place:
    def __init__(self, n):
        self.n = n
        self.side = side = math.isqrt(n // CORES)
        self.me = me = lax.axis_index("dp")
        self.core = lax.rem(me, CORES)
        self.y = lax.rem(lax.div(me, CORES), side)
        self.x = lax.div(me, CORES * side)
        self.twin = me + 1 - 2 * self.core

    def at(self, axis):
        return self.x if axis == 0 else self.y

    def along(self, axis, by):
        if axis == 0:
            return lax.rem(self.x + by + self.side, self.side) * (CORES * self.side) + self.y * CORES + self.core
        return self.x * (CORES * self.side) + lax.rem(self.y + by + self.side, self.side) * CORES + self.core

    def near(self):
        return [self.twin] + [self.along(axis, by) for axis in (0, 1) for by in (1, -1)]


def greet(devices):
    barrier = pltpu.get_barrier_semaphore()
    for d in devices:
        pl.semaphore_signal(barrier, inc=1, device_id={"dp": d}, device_id_type=pl.DeviceIdType.MESH)
    pl.semaphore_wait(barrier, len(devices))


def greet_all(place):
    barrier = pltpu.get_barrier_semaphore()

    def hello(k, _):
        pl.semaphore_signal(barrier, inc=1, device_id={"dp": lax.rem(place.me + k, place.n)}, device_id_type=pl.DeviceIdType.MESH)

    lax.fori_loop(1, place.n, hello, None)
    pl.semaphore_wait(barrier, place.n - 1)


def send(src, dst, sems, device):
    return pltpu.make_async_remote_copy(src, dst, sems[0], sems[1], device_id={"dp": device}, device_id_type=pl.DeviceIdType.MESH)


STREAMS = ((0, 1), (0, -1), (1, 1), (1, -1))


def stream_of(name, number):
    return {"w_up": 2, "w_down": 3}.get(name, number % 2)


class Scatter:
    def __init__(self, place, items, sems):
        self.p, self.items, self.send_s, self.recv_s, self.local_s = place, items, *sems
        self.pending = []

    @staticmethod
    def scratch(shapes, side):
        out = []
        for r, c in shapes:
            out += [pltpu.VMEM((side, side, r, c), jnp.bfloat16), pltpu.VMEM((side, side, r, c), jnp.bfloat16),
                    pltpu.VMEM((side - 1, side, r, c), jnp.bfloat16), pltpu.VMEM((side - 1, r, c), jnp.bfloat16)]
        return out

    def pair(self, i, k):
        return self.send_s.at[i, k], self.recv_s.at[i, k]

    def twin_copy(self, i):
        _, g, own, r0, r1, r2 = self.items[i]
        p = self.p
        return (send(g.at[:, :, 1 - p.core], r0, self.pair(i, 0), p.twin),
                pltpu.make_async_copy(g.at[:, :, p.core], own, self.local_s.at[i]))

    def ring_copy(self, i, stage, t):
        stream, g, own, r0, r1, r2 = self.items[i]
        p, (first, by) = self.p, STREAMS[stream]
        axis = first if stage == 0 else 1 - first
        block = lax.rem(p.at(axis) - by * (1 + t) + 2 * p.side, p.side)
        if stage == 0:
            src, dst = (own.at[block] if axis == 0 else own.at[:, block]), r1.at[t]
        else:
            src, dst = (own.at[block, p.y] if axis == 0 else own.at[p.x, block]), r2.at[t]
        return send(src, dst, self.pair(i, 1 + 3 * stage + t), p.along(axis, by))

    def start(self, i):
        for c in self.twin_copy(i):
            c.start()

    def join_twin(self, i):
        _, g, own, r0, r1, r2 = self.items[i]
        far, near = self.twin_copy(i)
        near.wait()
        far.wait()
        side = self.p.side

        def add(k, _):
            a, b = lax.div(k, side), lax.rem(k, side)
            own[a, b] = (own[a, b].astype(jnp.float32) + r0[a, b].astype(jnp.float32)).astype(own.dtype)

        lax.fori_loop(0, side * side, add, None)

    def hop(self, i, stage, t):
        self.ring_copy(i, stage, t).start()

    def join(self, i, stage, t):
        stream, g, own, r0, r1, r2 = self.items[i]
        p, (first, by) = self.p, STREAMS[stream]
        axis = first if stage == 0 else 1 - first
        self.ring_copy(i, stage, t).wait()
        block = lax.rem(p.at(axis) - by * (2 + t) + 2 * p.side, p.side)
        if stage == 0:
            def add(k, _):
                a, b = (block, k) if axis == 0 else (k, block)
                own[a, b] = (own[a, b].astype(jnp.float32) + r1[t, k].astype(jnp.float32)).astype(own.dtype)

            lax.fori_loop(0, p.side, add, None)
        elif t < p.side - 2:
            a, b = (block, p.y) if axis == 0 else (p.x, block)
            own[a, b] = (own[a, b].astype(jnp.float32) + r2[t].astype(jnp.float32)).astype(own.dtype)

    def result(self, i):
        _, g, own, r0, r1, r2 = self.items[i]
        p = self.p
        return (own[p.x, p.y].astype(jnp.float32) + r2[p.side - 2].astype(jnp.float32)).astype(own.dtype)


def scattered(grads, n):
    side = math.isqrt(n // CORES)
    count = len(grads)
    shapes = [(g.shape[0] // n, g.shape[1]) for _, _, g in grads]
    streams = [stream_of(name, number) for name, number, _ in grads]
    order = sorted(range(count), key=lambda i: (-(shapes[i][0] * shapes[i][1]), streams[i]))
    steps = side - 1

    def kernel(*refs):
        g_refs, out_refs, total_ref = refs[:count], refs[count : 2 * count], refs[2 * count]
        buffers, (send_s, recv_s, local_s, part, all_s, sq_send, sq_recv) = refs[2 * count + 1 : 6 * count + 1], refs[6 * count + 1 :]
        place = Place(n)
        greet_all(place)
        items = [(streams[i], g_refs[i], *buffers[4 * i : 4 * i + 4]) for i in range(count)]
        rs = Scatter(place, items, (send_s, recv_s, local_s))
        for i in order:
            rs.start(i)
        for i in order:
            rs.join_twin(i)
            rs.hop(i, 0, 0)
        for stage in range(2):
            for t in range(steps):
                for i in order:
                    rs.join(i, stage, t)
                    if t < steps - 1:
                        rs.hop(i, stage, t + 1)
                    elif stage == 0:
                        rs.hop(i, 1, 0)
        squares = jnp.zeros((8, 128), jnp.float32)
        for i in range(count):
            done = rs.result(i)
            out_refs[i][:] = done
            wide = done.astype(jnp.float32)
            squares += sum_tiles(wide * wide)
        everyone(place, squares, part, all_s, sq_send, sq_recv, total_ref)

    vmem = pl.BlockSpec(memory_space=pltpu.VMEM)
    outs = pl.pallas_call(
        kernel,
        in_specs=[pl.BlockSpec(memory_space=pl.ANY)] * count,
        out_specs=[vmem] * (count + 1),
        out_shape=[jax.ShapeDtypeStruct(s, jnp.bfloat16) for s in shapes] + [jax.ShapeDtypeStruct((8, 128), jnp.float32)],
        scratch_shapes=Scatter.scratch(shapes, side)
        + [pltpu.SemaphoreType.DMA((count, 1 + 2 * steps)), pltpu.SemaphoreType.DMA((count, 1 + 2 * steps)), pltpu.SemaphoreType.DMA((count,)),
           pltpu.VMEM((8, 128), jnp.float32), pltpu.VMEM((n, 8, 128), jnp.float32), pltpu.SemaphoreType.DMA((n,)), pltpu.SemaphoreType.DMA],
        compiler_params=pltpu.CompilerParams(collective_id=0, has_side_effects=True, vmem_limit_bytes=VMEM),
        name="scatter",
    )(*(g.reshape(side, side, CORES, *s) for (_, _, g), s in zip(grads, shapes)))
    return outs[:count], outs[count]


def sum_tiles(wide):
    rows, cols = wide.shape
    out = jnp.zeros((8, 128), jnp.float32)
    for a in range(0, rows, 8):
        for b in range(0, cols, 128):
            out = out + wide[a : a + 8, b : b + 128]
    return out


def everyone(place, mine, part, slots, send_s, recv_s, total_ref):
    part[:] = mine
    slots[place.me] = mine

    def copy(k):
        return send(part, slots.at[place.me], (send_s.at[k], recv_s), lax.rem(place.me + k, place.n))

    lax.fori_loop(1, place.n, lambda k, _: copy(k).start(), None)
    lax.fori_loop(1, place.n, lambda k, _: copy(k).wait_send(), None)
    pltpu.make_async_copy(slots.at[pl.ds(0, place.n - 1)], slots.at[pl.ds(0, place.n - 1)], recv_s).wait()
    total_ref[:] = lax.fori_loop(0, place.n, lambda k, so_far: so_far + slots[k], jnp.zeros((8, 128), jnp.float32))


def gathered(shards, n):
    side = math.isqrt(n // CORES)
    names = list(shards)
    steps = side - 1
    layers = shards[names[0]].shape[0]
    pieces = []
    for i, name in enumerate(names):
        if stream_of(name, 0) == stream_of(name, 1):
            pieces.append((i, 0, layers, stream_of(name, 0)))
        else:
            pieces += [(i, k, k + 1, stream_of(name, k)) for k in range(layers)]
    count, legs = len(pieces), steps + side * steps

    def kernel(*refs):
        mine, outs = refs[: len(names)], refs[len(names) : 2 * len(names)]
        send_s, recv_s, twin_send, twin_recv, local_s = refs[2 * len(names) :]
        place = Place(n)
        greet(place.near())

        def block(i, ref, p1, p2):
            array, a, b, stream = pieces[i]
            x, y = (p1, p2) if STREAMS[stream][0] == 0 else (p2, p1)
            return ref.at[pl.ds(a, b - a), x, y, place.core]

        def own(i):
            array, a, b, _ = pieces[i]
            return mine[array].at[pl.ds(a, b - a)]

        def spot(i, back1, back2):
            first, by = STREAMS[pieces[i][3]]
            return tuple(lax.rem(place.at(axis) - by * back + 2 * side, side) for axis, back in ((first, back1), (1 - first, back2)))

        def hop(i, leg, stage, back1, back2):
            first, by = STREAMS[pieces[i][3]]
            axis = first if stage == 0 else 1 - first
            out = outs[pieces[i][0]]
            at = block(i, out, *spot(i, back1, back2))
            return send(own(i) if back1 == back2 == 0 else at, at, (send_s.at[i, leg], recv_s.at[i, leg]), place.along(axis, by))

        def to_twin(i, k, back1, back2):
            at = block(i, outs[pieces[i][0]], *spot(i, back1, back2))
            return send(own(i) if back1 == back2 == 0 else at, at, (twin_send.at[i, k], twin_recv.at[i, k]), place.twin)

        def first_leg(t):
            return t

        def second_leg(j, t):
            return steps + j * steps + t

        started = []

        def go(copy):
            copy.start()
            started.append(copy)

        keep = [pltpu.make_async_copy(own(i), block(i, outs[pieces[i][0]], *spot(i, 0, 0)), local_s.at[i]) for i in range(count)]
        for i in range(count):
            go(hop(i, first_leg(0), 0, 0, 0))
            go(hop(i, second_leg(0, 0), 1, 0, 0))
        for i in range(count):
            keep[i].start()
            go(to_twin(i, 0, 0, 0))
        for k in range(2 * steps):
            for i in range(count):
                if k < steps:
                    hop(i, first_leg(k), 0, k, 0).wait_recv()
                    if k + 1 < steps:
                        go(hop(i, first_leg(k + 1), 0, k + 1, 0))
                    go(hop(i, second_leg(k + 1, 0), 1, k + 1, 0))
                    go(to_twin(i, (k + 1) * side, k + 1, 0))
                for j in range(side):
                    t = k - j
                    if 0 <= t < steps:
                        hop(i, second_leg(j, t), 1, j, t).wait_recv()
                        if t + 1 < steps:
                            go(hop(i, second_leg(j, t + 1), 1, j, t + 1))
                        go(to_twin(i, j * side + t + 1, j, t + 1))
        for i in range(count):
            keep[i].wait()
            for back1 in range(side):
                for back2 in range(side):
                    to_twin(i, back1 * side + back2, back1, back2).wait_recv()
        for copy in started:
            copy.wait_send()

    vmem = pl.BlockSpec(memory_space=pltpu.VMEM)
    outs = pl.pallas_call(
        kernel,
        in_specs=[vmem] * len(names),
        out_specs=[pl.BlockSpec(memory_space=pl.ANY)] * len(names),
        out_shape=[jax.ShapeDtypeStruct((layers, side, side, CORES, *s.shape[1:]), s.dtype) for s in shards.values()],
        scratch_shapes=[pltpu.SemaphoreType.DMA((count, legs)), pltpu.SemaphoreType.DMA((count, legs)),
                        pltpu.SemaphoreType.DMA((count, side * side)), pltpu.SemaphoreType.DMA((count, side * side)), pltpu.SemaphoreType.DMA((count,))],
        compiler_params=pltpu.CompilerParams(collective_id=1, has_side_effects=True),
        name="gather",
    )(*shards.values())
    return [out.reshape(layers, -1, out.shape[-1]) for out in outs]


def stepped(grads, total, weights, m, v, n, count):
    arrays = len(weights)
    layers = weights[0].shape[0]

    def kernel(me_ref, total_ref, *refs):
        g_refs, refs = refs[: arrays * layers], refs[arrays * layers :]
        w_refs, m_refs, v_refs, w_out, m_out, v_out = (refs[arrays * k : arrays * (k + 1)] for k in range(6))
        squares = jnp.sum(total_ref[:], keepdims=True)
        factor = jnp.minimum(1.0, 0.5 * lax.rsqrt(squares / count + 1e-30))
        for i in range(arrays):
            for k in range(layers):
                g = g_refs[i * layers + k][:].astype(jnp.float32) * factor
                new_m = 0.9 * m_refs[i][k] + 0.1 * g
                new_v = 0.95 * v_refs[i][k] + 0.05 * g * g
                w = w_refs[i][k, 0].astype(jnp.float32)
                step = new_m * lax.rsqrt(new_v + 1e-8) + 0.1 * w
                w_out[i][k] = (w - 0.02 * step).astype(jnp.bfloat16)
                m_out[i][k] = new_m
                v_out[i][k] = new_v

    whole = lambda a: pl.BlockSpec(a.shape, lambda i, me, nd=a.ndim: (0,) * nd)
    own = lambda a: pl.BlockSpec((a.shape[0], 1, a.shape[1] // n, a.shape[2]), lambda i, me: (0, me[0], 0, 0))
    flat = [g for pair in grads for g in pair]
    out = pl.pallas_call(
        kernel,
        grid_spec=pltpu.PrefetchScalarGridSpec(
            num_scalar_prefetch=1,
            grid=(1,),
            in_specs=[whole(total)] + [whole(g) for g in flat] + [own(w) for w in weights] + [whole(a) for a in (*m, *v)],
            out_specs=[whole(a) for a in (*m, *m, *v)],
        ),
        out_shape=[jax.ShapeDtypeStruct(a.shape, jnp.bfloat16) for a in m] + [jax.ShapeDtypeStruct(a.shape, a.dtype) for a in (*m, *v)],
        compiler_params=pltpu.CompilerParams(vmem_limit_bytes=VMEM),
        name="adamw",
    )(lax.axis_index("dp").reshape(1), total, *flat, *(w.reshape(w.shape[0], n, -1, w.shape[2]) for w in weights), *m, *v)
    return out[:arrays], out[arrays : 2 * arrays], out[2 * arrays :]


def gradients(x, dy, w, layers):
    tables = tables_of(x.shape[0])
    h, kept = x, []
    q, k, v = pre(h, tables, w, 0)
    for number in range(layers):
        o, lse = attend(q, k, v)
        if number < layers - 1:
            h2, gate, up, h3, *following = mid(h, o, tables, w, number)
            kept.append((h, q, k, v, o, lse, h2, (gate, up)))
            h, (q, k, v) = h3, following
        else:
            kept.append((h, q, k, v, o, lse, h, None))
    grads, by_h = [None] * layers, dy
    for number in reversed(range(layers)):
        h, q, k, v, o, lse, between, saved = kept[number]
        dh2, do, delta, gg, gu, gd, go = tail(between, o, by_h, w, number, saved)
        dq, dk, dv = attend_back(q, k, v, do, lse, delta)
        *rest, gq, gk, gv = back(h, dh2, dq, dk, dv, tables, w, number)
        by_h = rest[0] if rest else None
        grads[number] = dict(zip(NAMES, (gq, gk, gv, go, gg, gu, gd), strict=True))
    return grads


def solution(mesh):
    n = mesh.shape["dp"]

    def step(x, dy, *arrays):
        weights, m, v = (arrays[i : i + 7] for i in (0, 7, 14))
        layers = weights[0].shape[0]
        grads = gradients(x[0], dy[0], dict(zip(NAMES, weights, strict=True)), layers)
        terms = [(name, number, grads[number][name]) for name in NAMES for number in range(layers)]
        mine, total = scattered(terms, n)
        mine = [mine[layers * i : layers * (i + 1)] for i in range(7)]
        count = sum(w.size for w in weights)
        new_w, new_m, new_v = stepped(mine, total, weights, m, v, n, count)
        whole = gathered(dict(zip(NAMES, new_w, strict=True)), n)
        return (*whole, *new_m, *new_v)

    states, all_of, cut = P(("rep", "dp"), None, None), P(None, None, None), P(None, "dp", None)
    return jax.shard_map(
        step,
        mesh=mesh,
        in_specs=(states, states) + (all_of,) * 7 + (cut,) * 14,
        out_specs=(P("rep", None, None),) * 7 + (P("rep", "dp", None),) * 14,
        check_vma=False,
    )
```

```python
import functools
import math

import jax
import jax.numpy as jnp
from jax import lax
from jax.experimental import pallas as pl
from jax.experimental.pallas import tpu as pltpu
from jax.sharding import PartitionSpec as P

HEAD = 128
THETA = 10000
NAMES = ("wq", "wk", "wv", "wo", "w_gate", "w_up", "w_down")
NEG = -1e30
BIG = 1e30
LOG2E = 1.4426950408889634
VMEM = 56 * 2**20
MOST = 63 * 2**20
SMALL = 8 * 2**20


def dot(a, b):
    return jnp.dot(a, b, preferred_element_type=jnp.float32)


def dot_t(a, b):
    return lax.dot_general(a, b, (((1,), (1,)), ((), ())), preferred_element_type=jnp.float32)


def low(a):
    return a.astype(jnp.bfloat16)


def wide(a):
    return a.astype(jnp.float32)


def root(h):
    return lax.rsqrt(jnp.mean(h * h, -1, keepdims=True) + 1e-6)


def norm_back(h, r, by_a):
    return r * (by_a - h * (r * r * jnp.mean(h * by_a, -1, keepdims=True)))


def turned(t, cos, sin, way=1):
    other = pltpu.roll(t, HEAD // 2, 1) * sin
    return t * cos + other if way > 0 else t * cos - other


def heads_of(width):
    return [slice(at, at + HEAD) for at in range(0, width, HEAD)]


def parts_of(bt, size):
    return [slice(at, at + size) for at in range(0, bt, size)]


def project(part, a, wq, w_kv, cos_ref, sin_ref, q_ref, k_ref, v_ref):
    q, kv, cos, sin = low(dot(a, wq)), low(dot(a, w_kv)), cos_ref[part, :], sin_ref[part, :]
    for at in heads_of(q.shape[1]):
        q_ref[part, at] = low(turned(wide(q[:, at]), cos, sin))
    k_ref[part, :] = low(turned(wide(kv[:, :HEAD]), cos, sin))
    v_ref[part, :] = kv[:, HEAD:]


def _pre(h_ref, cos_ref, sin_ref, wq_ref, wk_ref, wv_ref, q_ref, k_ref, v_ref, w_kv, *, size):
    @pl.when(pl.program_id(0) == 0)
    def _():
        w_kv[:, :HEAD] = wk_ref[:]
        w_kv[:, HEAD:] = wv_ref[:]

    for part in parts_of(h_ref.shape[0], size):
        h = wide(h_ref[part, :])
        project(part, low(h * root(h)), wq_ref[:], w_kv[:], cos_ref, sin_ref, q_ref, k_ref, v_ref)


def rows(bt, width, last=None):
    return pl.BlockSpec((bt, width), lambda i: (i if last is None else jnp.minimum(i, last), 0))


def whole(shape, **more):
    return pl.BlockSpec(tuple(shape), lambda *_: (0,) * len(shape), **more)


def one_layer(w, number):
    return pl.BlockSpec((None, *w.shape[1:]), lambda i: (number, 0, 0), pipeline_mode=pl.Buffered(1))


def like(rows, cols, dtype=jnp.bfloat16):
    return jax.ShapeDtypeStruct((rows, cols), dtype)


def params():
    return pltpu.CompilerParams(dimension_semantics=("arbitrary",), vmem_limit_bytes=MOST)


def pre(h, tables, w, number, bt=512, size=256):
    tokens, d = h.shape
    wq, wk, wv = (w[name] for name in NAMES[:3])
    dk = wk.shape[2]
    return pl.pallas_call(
        functools.partial(_pre, size=size),
        grid=(tokens // bt,),
        in_specs=[rows(bt, d)] + [rows(bt, HEAD)] * 2 + [one_layer(a, number) for a in (wq, wk, wv)],
        out_specs=[rows(bt, wq.shape[2]), rows(bt, dk), rows(bt, dk)],
        out_shape=[like(tokens, wq.shape[2]), like(tokens, dk), like(tokens, dk)],
        scratch_shapes=[pltpu.VMEM((d, 2 * dk), jnp.bfloat16)],
        compiler_params=params(),
        name="pre",
    )(h, *tables, wq, wk, wv)


def gated(gate, up):
    return gate * jax.nn.sigmoid(gate) * up


def _mid(h_ref, o_ref, cos_ref, sin_ref, wo_ref, wg_ref, wu_ref, wd_ref, wq_ref, wk_ref, wv_ref,
         h2_ref, gate_ref, up_ref, h3_ref, q_ref, k_ref, v_ref, w_kv, s_s, *, cut, size):
    @pl.when(pl.program_id(0) == 0)
    def _():
        w_kv[:, :HEAD] = wk_ref[:]
        w_kv[:, HEAD:] = wv_ref[:]

    parts = parts_of(h_ref.shape[0], size)
    hs, bs = [], []
    for part in parts:
        h2 = low(wide(h_ref[part, :]) + wide(low(dot(o_ref[part, :], wo_ref[:]))))
        h2_ref[part, :] = h2
        h = wide(h2)
        hs.append(h2)
        bs.append(low(h * root(h)))
    for part, h, b in zip(parts, hs, bs):
        for f in range(0, wg_ref.shape[1], cut):
            at = slice(f, f + cut)
            gate, up = dot(b, wg_ref[:, at]), dot(b, wu_ref[:, at])
            gate_ref[part, at] = gate
            up_ref[part, at] = up
            s_s[part, at] = low(gated(gate, up))
        h3 = low(wide(h) + wide(low(dot(s_s[part, :], wd_ref[:]))))
        h3_ref[part, :] = h3
        h = wide(h3)
        project(part, low(h * root(h)), wq_ref[:], w_kv[:], cos_ref, sin_ref, q_ref, k_ref, v_ref)


def mid(h, o, tables, w, number, bt=512, cut=512, size=256):
    tokens, d = h.shape
    wq, wk, wv, wo, wg, wu, wd = (w[name] for name in NAMES)
    dk, ff = wk.shape[2], wg.shape[2]
    return pl.pallas_call(
        functools.partial(_mid, cut=cut, size=size),
        grid=(tokens // bt,),
        in_specs=[rows(bt, d), rows(bt, d)] + [rows(bt, HEAD)] * 2 + [one_layer(a, number) for a in (wo, wg, wu, wd)]
        + [one_layer(a, number + 1) for a in (wq, wk, wv)],
        out_specs=[rows(bt, d), rows(bt, ff), rows(bt, ff), rows(bt, d), rows(bt, wq.shape[2]), rows(bt, dk), rows(bt, dk)],
        out_shape=[like(tokens, d), like(tokens, ff, jnp.float32), like(tokens, ff, jnp.float32), like(tokens, d),
                   like(tokens, wq.shape[2]), like(tokens, dk), like(tokens, dk)],
        scratch_shapes=[pltpu.VMEM((d, 2 * dk), jnp.bfloat16), pltpu.VMEM((bt, ff), jnp.bfloat16)],
        compiler_params=params(),
        name="mid",
    )(h, o, *tables, wo, wg, wu, wd, wq, wk, wv)


def _tail(h_ref, o_ref, dy_ref, *rest, blocks, cut, out, size, saved):
    if saved:
        gate_ref, up_ref, *rest = rest
    (wo_ref, wg_ref, wu_ref, wd_ref, dh2_ref, do_ref, delta_ref, gg_ref, gu_ref, gd_ref, go_ref,
     b_t, dy_t, s_s, dgate_s, dup_s, go_s) = rest
    i = pl.program_id(0)
    bt, d = dy_ref.shape
    ff = wg_ref.shape[1]

    @pl.when(i == 0)
    def _():
        go_s[:] = jnp.zeros_like(go_s)

    @pl.when(i < blocks)
    def _():
        own = lax.div(lax.broadcasted_iota(jnp.int32, (8, d), 1), HEAD) == lax.broadcasted_iota(jnp.int32, (8, d), 0)
        pick = jnp.where(own, 1.0, 0.0).astype(jnp.bfloat16)
        state = []
        for part in parts_of(bt, size):
            h = wide(h_ref[part, :])
            if not saved:
                h = wide(low(h + wide(low(dot(o_ref[part, :], wo_ref[:])))))
            r = root(h)
            state.append((part, pl.ds(pl.multiple_of(i * bt + part.start, size), size), low(h), r, low(h * r)))
        for part, here, h, r, b in state:
            dy, o = dy_ref[part, :], o_ref[part, :]
            by_b = jnp.zeros((size, d), jnp.float32)
            for f in range(0, ff, cut):
                at = slice(f, f + cut)
                if saved:
                    gate, up = gate_ref[part, at], up_ref[part, at]
                else:
                    gate, up = dot(b, wg_ref[:, at]), dot(b, wu_ref[:, at])
                by_s = dot_t(dy, wd_ref[at, :])
                sig = jax.nn.sigmoid(gate)
                act = gate * sig
                s_s[here, at] = low(act * up)
                dup = low(by_s * act)
                dgate = low(by_s * up * (sig + act * (1 - sig)))
                dup_s[here, at] = dup
                dgate_s[here, at] = dgate
                by_b += dot_t(dgate, wg_ref[:, at]) + dot_t(dup, wu_ref[:, at])
            dh2 = low(wide(dy) + norm_back(wide(h), r, by_b))
            dh2_ref[part, :] = dh2
            do = low(dot_t(dh2, wo_ref[:]))
            do_ref[part, :] = do
            both = wide(do) * wide(o)
            first = low(both)
            second = low(both - wide(first))
            delta_ref[:, part] = dot_t(pick, first) + dot_t(pick, second)
            go_s[:] += dot(o.T, dh2)
            b_t[:, here] = b.T
            dy_t[:, here] = dy.T

    @pl.when(i >= blocks)
    def _():
        at = pl.ds(pl.multiple_of((i - blocks) * out, out), out)
        gg_ref[:] = low(dot(b_t[:], dgate_s[:, at]))
        gu_ref[:] = low(dot(b_t[:], dup_s[:, at]))
        gd_ref[:] = low(dot(dy_t[:], s_s[:, at]).T)

    @pl.when(i == pl.num_programs(0) - 1)
    def _():
        go_ref[:] = low(go_s[:])


def tail(h, o, dy, w, number, kept=None, bt=256, cut=512, out=256, size=256):
    tokens, d = dy.shape
    wo, wg, wu, wd = (w[name] for name in NAMES[3:])
    ff = wg.shape[2]
    blocks, last = tokens // bt, tokens // bt - 1
    after = lambda i: jnp.maximum(i - blocks, 0)
    return pl.pallas_call(
        functools.partial(_tail, blocks=blocks, cut=cut, out=out, size=size, saved=kept is not None),
        grid=(blocks + ff // out,),
        in_specs=[rows(bt, d, last)] * 3 + ([] if kept is None else [rows(bt, ff, last)] * 2) + [one_layer(a, number) for a in (wo, wg, wu, wd)],
        out_specs=[rows(bt, d, last), rows(bt, d, last), pl.BlockSpec((8, bt), lambda i: (0, jnp.minimum(i, last))),
                   pl.BlockSpec((d, out), lambda i: (0, after(i))), pl.BlockSpec((d, out), lambda i: (0, after(i))),
                   pl.BlockSpec((out, d), lambda i: (after(i), 0)), whole((d, d), pipeline_mode=pl.Buffered(1))],
        out_shape=[like(tokens, d), like(tokens, d), like(8, tokens, jnp.float32), like(d, ff), like(d, ff), like(ff, d), like(d, d)],
        scratch_shapes=[pltpu.VMEM((d, tokens), jnp.bfloat16)] * 2 + [pltpu.VMEM((tokens, ff), jnp.bfloat16)] * 3 + [pltpu.VMEM((d, d), jnp.float32)],
        compiler_params=params(),
        name="tail",
    )(h, o, dy, *(kept or ()), wo, wg, wu, wd)


def _back(h_ref, dh2_ref, dq_ref, dk_ref, dv_ref, cos_ref, sin_ref, wq_ref, wk_ref, wv_ref, *rest, blocks, size, first):
    dh_ref, rest = (None, rest) if first else (rest[0], rest[1:])
    gq_ref, gk_ref, gv_ref, a_t, d_s, w_kv = rest
    i = pl.program_id(0)

    @pl.when(i == 0)
    def _():
        w_kv[:, :HEAD] = wk_ref[:]
        w_kv[:, HEAD:] = wv_ref[:]

    bt, d = h_ref.shape
    dq_w = dq_ref.shape[1]
    for part in parts_of(bt, size):
        here = pl.ds(pl.multiple_of(i * bt + part.start, size), size)
        h = wide(h_ref[part, :])
        r = root(h)
        a_t[:, here] = low(h * r).T
        cos, sin = cos_ref[part, :], sin_ref[part, :]
        mine = [low(turned(wide(dq_ref[part, at]), cos, sin, -1)) for at in heads_of(dq_w)]
        mine += [low(turned(wide(dk_ref[part, :]), cos, sin, -1)), dv_ref[part, :]]
        mine = jnp.concatenate(mine, axis=1)
        d_s[here, :] = mine
        if not first:
            by_a = dot_t(mine[:, :dq_w], wq_ref[:]) + dot_t(mine[:, dq_w:], w_kv[:])
            dh_ref[part, :] = low(wide(dh2_ref[part, :]) + norm_back(h, r, by_a))

    @pl.when(i == blocks - 1)
    def _():
        got = low(dot(a_t[:], d_s[:]))
        gq_ref[:] = got[:, :dq_w]
        gk_ref[:] = got[:, dq_w : dq_w + HEAD]
        gv_ref[:] = got[:, dq_w + HEAD :]


def back(h, dh2, dq, dk, dv, tables, w, number, bt=512, size=256):
    tokens, d = h.shape
    wq, wk, wv = (w[name] for name in NAMES[:3])
    first = number == 0
    blocks = tokens // bt
    return pl.pallas_call(
        functools.partial(_back, blocks=blocks, size=size, first=first),
        grid=(blocks,),
        in_specs=[rows(bt, d), rows(bt, d), rows(bt, dq.shape[1]), rows(bt, HEAD), rows(bt, HEAD), rows(bt, HEAD), rows(bt, HEAD)]
        + [one_layer(a, number) for a in (wq, wk, wv)],
        out_specs=([] if first else [rows(bt, d)]) + [whole(a.shape[1:]) for a in (wq, wk, wv)],
        out_shape=([] if first else [like(tokens, d)]) + [like(*a.shape[1:]) for a in (wq, wk, wv)],
        scratch_shapes=[pltpu.VMEM((d, tokens), jnp.bfloat16), pltpu.VMEM((tokens, dq.shape[1] + 2 * HEAD), jnp.bfloat16), pltpu.VMEM((d, 2 * HEAD), jnp.bfloat16)],
        compiler_params=params(),
        name="back",
    )(h, dh2, dq, dk, dv, *tables, wq, wk, wv)


def tables_of(tokens, stride=64):
    half = HEAD // 2
    speed = THETA ** (-jnp.arange(half, dtype=jnp.float32) / half)

    def both(places):
        angle = places.astype(jnp.float32)[:, None] * speed
        return jnp.cos(angle), jnp.sin(angle)

    (c1, s1), (c2, s2) = both(jnp.arange(0, tokens, stride)), both(jnp.arange(stride))
    (c1, s1), (c2, s2) = (c1[:, None], s1[:, None]), (c2[None], s2[None])
    cos, sin = ((c1 * c2 - s1 * s2).reshape(tokens, half), (s1 * c2 + c1 * s2).reshape(tokens, half))
    return jnp.concatenate([cos, cos], 1), jnp.concatenate([-sin, sin], 1)


CORES = 2


class Place:
    def __init__(self, n):
        self.n = n
        self.side = side = math.isqrt(n // CORES)
        self.me = me = lax.axis_index("dp")
        self.core = lax.rem(me, CORES)
        self.y = lax.rem(lax.div(me, CORES), side)
        self.x = lax.div(me, CORES * side)
        self.twin = me + 1 - 2 * self.core

    def at(self, axis):
        return self.x if axis == 0 else self.y

    def along(self, axis, by):
        if axis == 0:
            return lax.rem(self.x + by + self.side, self.side) * (CORES * self.side) + self.y * CORES + self.core
        return self.x * (CORES * self.side) + lax.rem(self.y + by + self.side, self.side) * CORES + self.core

    def near(self):
        return [self.twin] + [self.along(axis, by) for axis in (0, 1) for by in (1, -1)]


def greet(devices):
    barrier = pltpu.get_barrier_semaphore()
    for d in devices:
        pl.semaphore_signal(barrier, inc=1, device_id={"dp": d}, device_id_type=pl.DeviceIdType.MESH)
    pl.semaphore_wait(barrier, len(devices))


def greet_all(place):
    barrier = pltpu.get_barrier_semaphore()

    def hello(k, _):
        pl.semaphore_signal(barrier, inc=1, device_id={"dp": lax.rem(place.me + k, place.n)}, device_id_type=pl.DeviceIdType.MESH)

    lax.fori_loop(1, place.n, hello, None)
    pl.semaphore_wait(barrier, place.n - 1)


def send(src, dst, sems, device):
    return pltpu.make_async_remote_copy(src, dst, sems[0], sems[1], device_id={"dp": device}, device_id_type=pl.DeviceIdType.MESH)


class Scatter:
    def __init__(self, place, pieces, g_refs, buffers, sems, out_refs):
        self.p, self.pieces, self.g_refs, self.out_refs = place, pieces, g_refs, out_refs
        self.buffers = [buffers[4 * i : 4 * i + 4] for i in range(len(pieces))]
        self.send_s, self.recv_s, self.local_s = sems
        self.half = place.side // 2

    @staticmethod
    def scratch(pieces, side):
        out, half = [], side // 2
        for _, r, c, *_ in pieces:
            r, c = r.stop - r.start, c.stop - c.start
            out += [pltpu.VMEM((side, side, r, c), jnp.bfloat16), pltpu.VMEM((side, side, r, c), jnp.bfloat16),
                    pltpu.VMEM((half, 2, side, r, c), jnp.bfloat16), pltpu.VMEM((half, 2, r, c), jnp.bfloat16)]
        count = len(pieces)
        return out, [pltpu.SemaphoreType.DMA((count, 1 + 4 * half)), pltpu.SemaphoreType.DMA((count, 1 + 4 * half)), pltpu.SemaphoreType.DMA((count,))]

    def pair(self, i, k):
        return self.send_s.at[i, k], self.recv_s.at[i, k]

    def twin_copies(self, i):
        g, r, c, *_ = self.pieces[i]
        g, (own, came, _, _), p = self.g_refs[g], self.buffers[i], self.p
        return (send(g.at[:, :, 1 - p.core, r, c], came, self.pair(i, 0), p.twin),
                pltpu.make_async_copy(g.at[:, :, p.core, r, c], own, self.local_s.at[i]))

    def start(self, i):
        for c in self.twin_copies(i):
            c.start()

    def join_twin(self, i):
        own, came, _, _ = self.buffers[i]
        far, near = self.twin_copies(i)
        near.wait()
        far.wait()

        def add(k, _):
            own[k] = low(wide(own[k]) + wide(came[k]))

        lax.fori_loop(0, self.p.side, add, None)

    def moves(self, i, stage, t):
        first = self.pieces[i][3]
        own, _, across, last = self.buffers[i]
        p, half = self.p, self.half
        axis = first if stage == 0 else 1 - first
        away = half - t
        cols = own.shape[3]
        out = []
        for way, by in enumerate((1, -1)):
            to = lax.rem(p.at(axis) + by * away + p.side, p.side)
            into = lax.rem(p.at(axis) + by * (away - 1) + p.side, p.side)
            if stage == 0:
                part = pl.ds(way * half, half) if away == half else pl.ds(0, p.side)
                view = lambda k: own.at[k, part] if axis == 0 else own.at[part, k]
                arrived = across.at[t, way, pl.ds(0, part.size)]
            else:
                if away < half:
                    part = pl.ds(0, cols)
                elif cols >= 256:
                    middle = cols // 256 * 128
                    part = pl.ds(0, middle) if way == 0 else pl.ds(middle, cols - middle)
                elif way == 0:
                    part = pl.ds(0, cols)
                else:
                    continue
                view = lambda k: own.at[k, p.y, :, part] if axis == 0 else own.at[p.x, k, :, part]
                arrived = last.at[t, way, :, pl.ds(0, part.size)]
            copy = send(view(to), arrived, self.pair(i, 1 + 2 * half * stage + 2 * t + way), p.along(axis, by))
            out.append((copy, view(into), arrived))
        return out

    def hop(self, i, stage, t):
        for copy, _, _ in self.moves(i, stage, t):
            copy.start()

    def join(self, i, stage, t):
        moves = self.moves(i, stage, t)
        for copy, _, _ in moves:
            copy.wait()
        if t == self.half - 1 and self.half > 1:
            moves = [(moves[0][1], [arrived for _, _, arrived in moves])]
        else:
            moves = [(into, [arrived]) for _, into, arrived in moves]
        for into, arrived in moves:
            total = wide(into[:])
            for a in arrived:
                total += wide(a[:])
            into[:] = low(total)

    def phase(self, k, group, squares):
        for i in group:
            if k == 0:
                self.start(i)
            elif k == 1:
                self.join_twin(i)
                self.hop(i, 0, 0)
            else:
                stage, t = (k - 2) // self.half, (k - 2) % self.half
                self.join(i, stage, t)
                if k < 1 + 2 * self.half:
                    self.hop(i, (k - 1) // self.half, (k - 1) % self.half)
                else:
                    done = self.buffers[i][0][self.p.x, self.p.y]
                    self.out_refs[i][:] = done
                    squares[:] += sum_tiles(wide(done) * wide(done))

    @property
    def last(self):
        return 1 + 2 * self.half


def pieces_of(names, shapes, n):
    out = []
    for g, (name, (rows, cols)) in enumerate(zip(names, shapes)):
        r, c, middle = slice(0, rows // n), slice(0, cols), cols // 2
        halves = [slice(0, middle), slice(middle, cols)]
        if name in ("w_gate", "w_up"):
            out += [(g, r, part, int(name == "w_up"), group) for group, part in enumerate(halves)]
        elif name == "w_down":
            out += [(g, part, c, axis, 2) for axis, part in enumerate((slice(0, r.stop // 2), slice(r.stop // 2, r.stop)))]
        elif cols > HEAD:
            out += [(g, r, part, axis, 3) for axis, part in enumerate(halves)]
        else:
            out.append((g, r, c, int(name == "wv"), 3))
    return out


def blocked(g, n):
    side = math.isqrt(n // CORES)
    return g.reshape(side, side, CORES, g.shape[0] // n, g.shape[1])


def piece_shape(piece):
    return jax.ShapeDtypeStruct((piece[1].stop - piece[1].start, piece[2].stop - piece[2].start), jnp.bfloat16)


def finished(terms, squares, n):
    side = math.isqrt(n // CORES)
    pieces = pieces_of([name for name, _, _ in terms], [g.shape for _, _, g in terms], n)
    count = len(pieces)
    buffers, sems = Scatter.scratch(pieces, side)

    def kernel(*refs):
        g_refs, squares_refs, refs = refs[: len(terms)], refs[len(terms) : len(terms) + len(squares)], refs[len(terms) + len(squares) :]
        out_refs, total_ref, refs = refs[:count], refs[count], refs[count + 1 :]
        own, (send_s, recv_s, local_s, part, slots, sq_send, sq_recv) = refs[: len(buffers)], refs[len(buffers) :]
        place = Place(n)
        greet_all(place)
        rs = Scatter(place, pieces, g_refs, own, (send_s, recv_s, local_s), out_refs)
        part[:] = sum(ref[:] for ref in squares_refs)
        for k in range(rs.last + 1):
            rs.phase(k, range(count), part)
        everyone(place, part, slots, sq_send, sq_recv, total_ref)

    vmem = pl.BlockSpec(memory_space=pltpu.VMEM)
    outs = pl.pallas_call(
        kernel,
        in_specs=[pl.BlockSpec(memory_space=pl.ANY)] * len(terms) + [vmem] * len(squares),
        out_specs=[vmem] * (count + 1),
        out_shape=[piece_shape(p) for p in pieces] + [like(8, HEAD, jnp.float32)],
        scratch_shapes=buffers + sems
        + [pltpu.VMEM((8, HEAD), jnp.float32), pltpu.VMEM((n, 8, HEAD), jnp.float32), pltpu.SemaphoreType.DMA((n,)), pltpu.SemaphoreType.DMA],
        compiler_params=pltpu.CompilerParams(collective_id=0, has_side_effects=True, vmem_limit_bytes=VMEM),
        name="finish",
    )(*(blocked(g, n) for _, _, g in terms), *squares)
    return list(zip(pieces, outs)), outs[count]


def sum_tiles(wide):
    rows, cols = wide.shape
    out = jnp.zeros((8, 128), jnp.float32)
    for a in range(0, rows, 8):
        for b in range(0, cols, 128):
            out = out + wide[a : a + 8, b : b + 128]
    return out


def everyone(place, part, slots, send_s, recv_s, total_ref):
    slots[place.me] = part[:]

    def copy(k):
        return send(part, slots.at[place.me], (send_s.at[k], recv_s), lax.rem(place.me + k, place.n))

    lax.fori_loop(1, place.n, lambda k, _: copy(k).start(), None)
    lax.fori_loop(1, place.n, lambda k, _: copy(k).wait_send(), None)
    pltpu.make_async_copy(slots.at[pl.ds(0, place.n - 1)], slots.at[pl.ds(0, place.n - 1)], recv_s).wait()
    total_ref[:] = lax.fori_loop(0, place.n, lambda k, so_far: so_far + slots[k], jnp.zeros_like(part))


STREAMS = ((0, 1), (0, -1), (1, 1), (1, -1))


def stream_of(name, number):
    return {"w_up": 2, "w_down": 3}.get(name, number % 2)


def settled(arrays):
    count = len(arrays)

    def kernel(*refs):
        sems = refs[2 * count]
        copies = [pltpu.make_async_copy(refs[i], refs[count + i], sems.at[i]) for i in range(count)]
        for c in copies:
            c.start()
        for c in copies:
            c.wait()

    return pl.pallas_call(
        kernel,
        in_specs=[pl.BlockSpec(memory_space=pltpu.VMEM)] * count,
        out_specs=[pl.BlockSpec(memory_space=pltpu.HBM)] * count,
        out_shape=[jax.ShapeDtypeStruct(a.shape, a.dtype) for a in arrays],
        scratch_shapes=[pltpu.SemaphoreType.DMA((count,))],
        compiler_params=pltpu.CompilerParams(vmem_limit_bytes=SMALL),
        name="settle",
    )(*arrays)


def gathered(shards, n):
    side = math.isqrt(n // CORES)
    names = list(shards)
    steps = side - 1
    layers = shards[names[0]].shape[0]
    pieces = []
    for i, name in enumerate(names):
        if stream_of(name, 0) == stream_of(name, 1):
            pieces.append((i, 0, layers, stream_of(name, 0)))
        else:
            pieces += [(i, k, k + 1, stream_of(name, k)) for k in range(layers)]
    count, legs = len(pieces), steps + side * steps

    def kernel(*refs):
        mine, outs = refs[: len(names)], refs[len(names) : 2 * len(names)]
        send_s, recv_s, twin_send, twin_recv, local_s = refs[2 * len(names) :]
        place = Place(n)
        greet(place.near())

        def block(i, ref, p1, p2):
            array, a, b, stream = pieces[i]
            x, y = (p1, p2) if STREAMS[stream][0] == 0 else (p2, p1)
            return ref.at[pl.ds(a, b - a), x, y, place.core]

        def own(i):
            array, a, b, _ = pieces[i]
            return mine[array].at[pl.ds(a, b - a)]

        def spot(i, back1, back2):
            first, by = STREAMS[pieces[i][3]]
            return tuple(lax.rem(place.at(axis) - by * back + 2 * side, side) for axis, back in ((first, back1), (1 - first, back2)))

        def hop(i, leg, stage, back1, back2):
            first, by = STREAMS[pieces[i][3]]
            axis = first if stage == 0 else 1 - first
            out = outs[pieces[i][0]]
            at = block(i, out, *spot(i, back1, back2))
            return send(own(i) if back1 == back2 == 0 else at, at, (send_s.at[i, leg], recv_s.at[i, leg]), place.along(axis, by))

        def to_twin(i, k, back1, back2):
            at = block(i, outs[pieces[i][0]], *spot(i, back1, back2))
            return send(own(i) if back1 == back2 == 0 else at, at, (twin_send.at[i, k], twin_recv.at[i, k]), place.twin)

        def first_leg(t):
            return t

        def second_leg(j, t):
            return steps + j * steps + t

        started = []

        def go(copy):
            copy.start()
            started.append(copy)

        keep = [pltpu.make_async_copy(own(i), block(i, outs[pieces[i][0]], *spot(i, 0, 0)), local_s.at[i]) for i in range(count)]
        for i in range(count):
            go(hop(i, first_leg(0), 0, 0, 0))
            go(hop(i, second_leg(0, 0), 1, 0, 0))
        for i in range(count):
            keep[i].start()
            go(to_twin(i, 0, 0, 0))
        for k in range(2 * steps):
            for i in range(count):
                if k < steps:
                    hop(i, first_leg(k), 0, k, 0).wait_recv()
                    if k + 1 < steps:
                        go(hop(i, first_leg(k + 1), 0, k + 1, 0))
                    go(hop(i, second_leg(k + 1, 0), 1, k + 1, 0))
                    go(to_twin(i, (k + 1) * side, k + 1, 0))
                for j in range(side):
                    t = k - j
                    if 0 <= t < steps:
                        hop(i, second_leg(j, t), 1, j, t).wait_recv()
                        if t + 1 < steps:
                            go(hop(i, second_leg(j, t + 1), 1, j, t + 1))
                        go(to_twin(i, j * side + t + 1, j, t + 1))
        for i in range(count):
            keep[i].wait()
            for back1 in range(side):
                for back2 in range(side):
                    to_twin(i, back1 * side + back2, back1, back2).wait_recv()
        for copy in started:
            copy.wait_send()

    vmem = pl.BlockSpec(memory_space=pltpu.VMEM)
    outs = pl.pallas_call(
        kernel,
        in_specs=[vmem] * len(names),
        out_specs=[vmem] * len(names),
        out_shape=[pltpu.VMEM((layers, side, side, CORES, *s.shape[1:]), s.dtype) for s in shards.values()],
        scratch_shapes=[pltpu.SemaphoreType.DMA((count, legs)), pltpu.SemaphoreType.DMA((count, legs)),
                        pltpu.SemaphoreType.DMA((count, side * side)), pltpu.SemaphoreType.DMA((count, side * side)), pltpu.SemaphoreType.DMA((count,))],
        compiler_params=pltpu.CompilerParams(collective_id=1, has_side_effects=True, vmem_limit_bytes=SMALL),
        name="gather",
    )(*shards.values())
    return settled([out.reshape(layers, -1, out.shape[-1]) for out in outs])


def stepped(pieces, total, weights, m, v, n, count):
    arrays = len(weights)

    def kernel(me_ref, total_ref, *refs):
        g_refs, refs = refs[: len(pieces)], refs[len(pieces) :]
        w_refs, m_refs, v_refs, w_out, m_out, v_out = (refs[arrays * k : arrays * (k + 1)] for k in range(6))
        squares = jnp.sum(total_ref[:], keepdims=True)
        factor = jnp.minimum(1.0, 0.5 * lax.rsqrt(squares / count + 1e-30))
        for (i, k, r, c, _), g_ref in zip(pieces, g_refs):
            g = wide(g_ref[:]) * factor
            new_m = 0.9 * m_refs[i][k, r, c] + 0.1 * g
            new_v = 0.95 * v_refs[i][k, r, c] + 0.05 * g * g
            w = wide(w_refs[i][k, 0, r, c])
            step = new_m * lax.rsqrt(new_v + 1e-8) + 0.1 * w
            w_out[i][k, r, c] = low(w - 0.02 * step)
            m_out[i][k, r, c] = new_m
            v_out[i][k, r, c] = new_v

    own = lambda a: pl.BlockSpec((a.shape[0], 1, a.shape[1] // n, a.shape[2]), lambda i, me: (0, me[0], 0, 0))
    flat = [g for *_, g in pieces]
    out = pl.pallas_call(
        kernel,
        grid_spec=pltpu.PrefetchScalarGridSpec(
            num_scalar_prefetch=1,
            grid=(1,),
            in_specs=[whole(total.shape)] + [whole(g.shape) for g in flat] + [own(w) for w in weights] + [whole(a.shape) for a in (*m, *v)],
            out_specs=[pl.BlockSpec(memory_space=pltpu.VMEM)] * arrays + [whole(a.shape) for a in (*m, *v)],
        ),
        out_shape=[pltpu.VMEM(a.shape, jnp.bfloat16) for a in m] + [jax.ShapeDtypeStruct(a.shape, a.dtype) for a in (*m, *v)],
        compiler_params=pltpu.CompilerParams(vmem_limit_bytes=VMEM),
        name="adamw",
    )(lax.axis_index("dp").reshape(1), total, *flat, *(w.reshape(w.shape[0], n, -1, w.shape[2]) for w in weights), *m, *v)
    return out[:arrays], out[arrays : 2 * arrays], out[2 * arrays :]


def cut_off(keys, queries, ahead=0):
    return lax.broadcasted_iota(jnp.int32, (keys, queries), 1) >= lax.broadcasted_iota(jnp.int32, (keys, queries), 0) + ahead


def _forward(q_ref, k_ref, v_ref, o_ref, lse_ref, base_s, mix_s, *, part, e):
    bq, width = q_ref.shape
    heads = heads_of(width)
    iq = pl.program_id(0)

    def values(here, count):
        return jnp.concatenate([v_ref[here, :].T, jnp.ones((8, count), jnp.bfloat16)], axis=0)

    def block(at, count, seen, masked):
        here = pl.ds(pl.multiple_of(at, count), count)
        k, mixed = k_ref[here, :], values(here, count)
        score = lambda n: dot_t(k, q_ref[seen:, heads[n]])

        def weight(n, s):
            p = jnp.exp2(s * e - base_s[n : n + 1, seen:])
            return low(jnp.where(cut_off(count, bq - seen), p, 0.0) if masked else p)

        last = len(heads) - 1
        s, p = score(0), None
        for n in range(last + 2):
            following = score(n + 1) if n < last else None
            new = weight(n, s) if n <= last else None
            if n > 0:
                mix_s[n - 1, :, seen:] += dot(mixed, p)
            s, p = following, new

    for n, head in enumerate(heads):
        base_s[n : n + 1, :] = dot_t(k_ref[:8, :], q_ref[:, head])[:1] * e
    mix_s[:] = jnp.zeros_like(mix_s)
    lax.fori_loop(0, iq, lambda j, _: block(j * bq, bq, 0, False), None)
    for at in range(0, bq, part):
        block(iq * bq + at, part, at, True)

    @pl.when(jnp.sum(jnp.where(jnp.abs(mix_s[:]) < BIG, 0.0, 1.0)) > 0)
    def _():
        def again(j, n):
            here = pl.ds(pl.multiple_of(j * bq, bq), bq)
            head = pl.ds(pl.multiple_of(n * HEAD, HEAD), HEAD)
            s = jnp.where(cut_off(bq, bq, (j - iq) * bq), dot_t(k_ref[here, :], q_ref[:, head]) * e, 2 * NEG)
            old = base_s[pl.ds(n, 1), :]
            top = jnp.maximum(old, s.max(axis=0, keepdims=True))
            base_s[pl.ds(n, 1), :] = top
            mix_s[n] = mix_s[n] * jnp.exp2(old - top) + dot(values(here, bq), low(jnp.exp2(s - top)))
            return n

        base_s[:] = jnp.full_like(base_s, NEG)
        mix_s[:] = jnp.zeros_like(mix_s)
        lax.fori_loop(0, len(heads), lambda n, _: lax.fori_loop(0, iq + 1, again, n), 0)

    for n, head in enumerate(heads):
        total = mix_s[n, HEAD : HEAD + 1, :]
        o_ref[:, head] = low((mix_s[n, :HEAD, :] * (1 / total)).T)
        lse_ref[n : n + 1, :] = base_s[n : n + 1, :] + jnp.log(total) * LOG2E


def attend(q, k, v, bq=1024, part=256):
    tokens, width = q.shape
    heads = width // HEAD
    every_key = whole((tokens, HEAD))
    return pl.pallas_call(
        functools.partial(_forward, part=part, e=HEAD**-0.5 * LOG2E),
        grid=(tokens // bq,),
        in_specs=[rows(bq, width), every_key, every_key],
        out_specs=[rows(bq, width), pl.BlockSpec((8, bq), lambda i: (0, i))],
        out_shape=[like(tokens, width), like(8, tokens, jnp.float32)],
        scratch_shapes=[pltpu.VMEM((8, bq), jnp.float32), pltpu.VMEM((heads, HEAD + 8, bq), jnp.float32)],
        compiler_params=params(),
        name="attend",
    )(q, k, v)


WHEN = ((0, 2, 4, 7, 12, 16), (0, 3, 5, 10, 14, 17), (0, 4, 8, 14, 16, 18), (0, 6, 11, 16, 17, 19))


def attend_back(q, k, v, do, lse, delta, terms, n, number, bq=512, part=256):
    tokens, width = q.shape
    heads, e = heads_of(width), HEAD**-0.5 * LOG2E
    blocks, scale = tokens // bq, HEAD**-0.5
    steps = blocks * (blocks + 1) // 2
    side = math.isqrt(n // CORES)
    pieces = pieces_of([name for name, _, _ in terms], [g.shape for _, _, g in terms], n)
    count = len(pieces)
    buffers, sems = Scatter.scratch(pieces, side)
    groups = [[i for i, p in enumerate(pieces) if p[4] == group] for group in range(4)]

    def block_of(i):
        return sum(jnp.where(i >= row * (row + 1) // 2, 1, 0) for row in range(1, blocks))

    def kernel(q_ref, k_ref, v_ref, do_ref, lse_ref, delta_ref, *refs):
        g_refs, (dq_ref, dk_ref, dv_ref, *refs) = refs[: len(terms)], refs[len(terms) :]
        out_refs, squares_ref, (dq_s, dk_s, dv_s, *refs) = refs[:count], refs[count], refs[count + 1 :]
        i = pl.program_id(0)
        iq = block_of(i)
        j = i - lax.div(iq * (iq + 1), 2)
        place = Place(n)
        rs = Scatter(place, pieces, g_refs, refs[: len(buffers)], refs[len(buffers) :], out_refs)

        @pl.when(i == 0)
        def _():
            greet(place.near())
            dk_s[:] = jnp.zeros_like(dk_s)
            dv_s[:] = jnp.zeros_like(dv_s)
            squares_ref[:] = jnp.zeros_like(squares_ref)

        def beside(late, steps_here):
            for at in steps_here:
                todo = [(phase, group) for group, times in zip(groups, WHEN) for phase, time in enumerate(times) if time == 2 * at + late]
                if todo:
                    @pl.when(i == at)
                    def _():
                        for phase, group in todo:
                            rs.phase(phase, group, squares_ref)

        beside(0, range(steps))

        @pl.when(j == 0)
        def _():
            dq_s[:] = jnp.zeros_like(dq_s)

        def block(at, size, seen, masked, some):
            here = pl.ds(pl.multiple_of(at, size), size)
            k, v = k_ref[here, :], v_ref[here, :]
            k_t = k.T
            ok = cut_off(size, bq - seen) if masked else None
            scores = [dot_t(k, q_ref[seen:, head]) for _, head in some]
            dps = [dot_t(v, do_ref[seen:, head]) for _, head in some]
            for (n, head), s, dp in zip(some, scores, dps):
                p = jnp.exp2(s * e - lse_ref[n : n + 1, seen:])
                if masked:
                    p = jnp.where(ok, p, 0.0)
                ds = low(p * (dp - delta_ref[n : n + 1, seen:]))
                dv_s[here, :] += dot(low(p), do_ref[seen:, head])
                dk_s[here, :] += dot(ds, q_ref[seen:, head])
                dq_s[n, :, seen:] += dot(k_t, ds)

        every = list(enumerate(heads))
        ends = [row * (row + 3) // 2 for row in range(blocks)]

        @pl.when(j < iq)
        def _():
            block(j * bq, bq, 0, False, every[: len(every) // 2])
            beside(1, [at for at in range(steps) if at not in ends])
            block(j * bq, bq, 0, False, every[len(every) // 2 :])

        @pl.when(j == iq)
        def _():
            block(j * bq, part, 0, True, every)
            beside(1, ends)
            for seen in range(part, bq, part):
                block(j * bq + seen, part, seen, True, every)
            for n, head in every:
                dq_ref[:, head] = low((dq_s[n] * scale).T)

        @pl.when(i == steps - 1)
        def _():
            for phase in range(rs.last + 1):
                for group, times in zip(groups, WHEN):
                    if times[phase] >= 2 * steps:
                        rs.phase(phase, group, squares_ref)
            dk_ref[:] = low(dk_s[:] * scale)
            dv_ref[:] = low(dv_s[:])

    every_key = whole((tokens, HEAD))
    mine = pl.BlockSpec((bq, width), lambda i: (block_of(i), 0))
    stats = pl.BlockSpec((8, bq), lambda i: (0, block_of(i)))
    sums = [piece_shape(p) for p in pieces] + [like(8, HEAD, jnp.float32)]
    dq, dk, dv, *outs = pl.pallas_call(
        kernel,
        grid=(steps,),
        in_specs=[mine, every_key, every_key, mine, stats, stats] + [pl.BlockSpec(memory_space=pl.ANY)] * len(terms),
        out_specs=[mine, every_key, every_key] + [whole(s.shape) for s in sums],
        out_shape=[like(tokens, width), like(tokens, HEAD), like(tokens, HEAD)] + sums,
        scratch_shapes=[pltpu.VMEM((len(heads), HEAD, bq), jnp.float32), pltpu.VMEM((tokens, HEAD), jnp.float32), pltpu.VMEM((tokens, HEAD), jnp.float32)]
        + buffers + sems,
        compiler_params=pltpu.CompilerParams(dimension_semantics=("arbitrary",), vmem_limit_bytes=MOST, collective_id=2 + number, has_side_effects=True),
        name="attend_back",
    )(q, k, v, do, lse, delta, *(blocked(g, n) for _, _, g in terms))
    return dq, dk, dv, list(zip(pieces, outs)), outs[count]


def summed(x, dy, w, n):
    tables = tables_of(x.shape[0])
    layers = w["wq"].shape[0]
    h, kept = x, []
    q, k, v = pre(h, tables, w, 0)
    for number in range(layers):
        o, lse = attend(q, k, v)
        if number < layers - 1:
            h2, gate, up, h3, *following = mid(h, o, tables, w, number)
            kept.append((h, q, k, v, o, lse, h2, (gate, up)))
            h, (q, k, v) = h3, following
        else:
            kept.append((h, q, k, v, o, lse, h, None))
    by_h, waiting, sums, squares = dy, [], [], []

    def note(terms, got):
        for (g, r, c, *_), block in got:
            sums.append((NAMES.index(terms[g][0]), terms[g][1], r, c, block))

    for number in reversed(range(layers)):
        h, q, k, v, o, lse, between, saved = kept[number]
        dh2, do, delta, gg, gu, gd, go = tail(between, o, by_h, w, number, saved)
        terms = [(name, number, g) for name, g in zip(NAMES[4:] + NAMES[3:4], (gg, gu, gd, go))] + waiting
        dq, dk, dv, got, some = attend_back(q, k, v, do, lse, delta, terms, n, number)
        note(terms, got)
        squares.append(some)
        *rest, gq, gk, gv = back(h, dh2, dq, dk, dv, tables, w, number)
        by_h = rest[0] if rest else None
        waiting = [(name, number, g) for name, g in zip(NAMES[:3], (gq, gk, gv))]
    got, total = finished(waiting, squares, n)
    note(waiting, got)
    return sums, total


def solution(mesh):
    n = mesh.shape["dp"]

    def step(x, dy, *arrays):
        weights, m, v = (arrays[i : i + 7] for i in (0, 7, 14))
        sums, total = summed(x[0], dy[0], dict(zip(NAMES, weights)), n)
        new_w, new_m, new_v = stepped(sums, total, weights, m, v, n, sum(w.size for w in weights))
        whole = gathered(dict(zip(NAMES, new_w)), n)
        return (*whole, *new_m, *new_v)

    states, all_of, cut = P(("rep", "dp"), None, None), P(None, None, None), P(None, "dp", None)
    return jax.shard_map(
        step,
        mesh=mesh,
        in_specs=(states, states) + (all_of,) * 7 + (cut,) * 14,
        out_specs=(P("rep", None, None),) * 7 + (P("rep", "dp", None),) * 14,
        check_vma=False,
    )
```

```python
import functools
import math

import jax
import jax.numpy as jnp
from jax import lax
from jax.experimental import pallas as pl
from jax.experimental.pallas import tpu as pltpu
from jax.sharding import PartitionSpec as P

HEAD = 128
THETA = 10000
NAMES = ("wq", "wk", "wv", "wo", "w_gate", "w_up", "w_down")
NEG = -1e30
BIG = 1e30
LOG2E = 1.4426950408889634
VMEM = 56 * 2**20
MOST = 63 * 2**20
SMALL = 8 * 2**20


def dot(a, b):
    return jnp.dot(a, b, preferred_element_type=jnp.float32)


def dot_t(a, b):
    return lax.dot_general(a, b, (((1,), (1,)), ((), ())), preferred_element_type=jnp.float32)


def low(a):
    return a.astype(jnp.bfloat16)


def wide(a):
    return a.astype(jnp.float32)


def root(h):
    return lax.rsqrt(jnp.mean(h * h, -1, keepdims=True) + 1e-6)


def norm_back(h, r, by_a):
    return r * (by_a - h * (r * r * jnp.mean(h * by_a, -1, keepdims=True)))


def turned(t, cos, sin, way=1):
    other = pltpu.roll(t, HEAD // 2, 1) * sin
    return t * cos + other if way > 0 else t * cos - other


def heads_of(width):
    return [slice(at, at + HEAD) for at in range(0, width, HEAD)]


def parts_of(bt, size):
    return [slice(at, at + size) for at in range(0, bt, size)]


def project(part, a, wq, w_kv, cos_ref, sin_ref, q_ref, k_ref, v_ref):
    q, kv, cos, sin = low(dot(a, wq)), low(dot(a, w_kv)), cos_ref[part, :], sin_ref[part, :]
    for at in heads_of(q.shape[1]):
        q_ref[part, at] = low(turned(wide(q[:, at]), cos, sin))
    k_ref[part, :] = low(turned(wide(kv[:, :HEAD]), cos, sin))
    v_ref[part, :] = kv[:, HEAD:]


def _pre(h_ref, cos_ref, sin_ref, wq_ref, wk_ref, wv_ref, q_ref, k_ref, v_ref, w_kv):
    @pl.when(pl.program_id(0) == 0)
    def _():
        w_kv[:, :HEAD] = wk_ref[:]
        w_kv[:, HEAD:] = wv_ref[:]

    h = wide(h_ref[:])
    project(slice(None), low(h * root(h)), wq_ref[:], w_kv[:], cos_ref, sin_ref, q_ref, k_ref, v_ref)


def rows(bt, width, last=None):
    return pl.BlockSpec((bt, width), lambda i: (i if last is None else jnp.minimum(i, last), 0))


def whole(shape, **more):
    return pl.BlockSpec(tuple(shape), lambda *_: (0,) * len(shape), **more)


def one_layer(w, number):
    return pl.BlockSpec((None, *w.shape[1:]), lambda i: (number, 0, 0), pipeline_mode=pl.Buffered(1))


def like(rows, cols, dtype=jnp.bfloat16):
    return jax.ShapeDtypeStruct((rows, cols), dtype)


def params():
    return pltpu.CompilerParams(dimension_semantics=("arbitrary",), vmem_limit_bytes=MOST)


def pre(h, tables, w, number, bt=512):
    tokens, d = h.shape
    wq, wk, wv = (w[name] for name in NAMES[:3])
    dk = wk.shape[2]
    return pl.pallas_call(
        _pre,
        grid=(tokens // bt,),
        in_specs=[rows(bt, d)] + [rows(bt, HEAD)] * 2 + [one_layer(a, number) for a in (wq, wk, wv)],
        out_specs=[rows(bt, wq.shape[2]), rows(bt, dk), rows(bt, dk)],
        out_shape=[like(tokens, wq.shape[2]), like(tokens, dk), like(tokens, dk)],
        scratch_shapes=[pltpu.VMEM((d, 2 * dk), jnp.bfloat16)],
        compiler_params=params(),
        name="pre",
    )(h, *tables, wq, wk, wv)


def gated(gate, up):
    return gate * jax.nn.sigmoid(gate) * up


def _mid(h_ref, o_ref, cos_ref, sin_ref, wo_ref, wg_ref, wu_ref, wd_ref, wq_ref, wk_ref, wv_ref,
         h2_ref, gate_ref, up_ref, h3_ref, q_ref, k_ref, v_ref, w_kv, s_s, *, cut, size):
    @pl.when(pl.program_id(0) == 0)
    def _():
        w_kv[:, :HEAD] = wk_ref[:]
        w_kv[:, HEAD:] = wv_ref[:]

    parts = parts_of(h_ref.shape[0], size)
    hs, bs = [], []
    for part in parts:
        h2 = low(wide(h_ref[part, :]) + wide(low(dot(o_ref[part, :], wo_ref[:]))))
        h2_ref[part, :] = h2
        h = wide(h2)
        hs.append(h2)
        bs.append(low(h * root(h)))
    for part, h, b in zip(parts, hs, bs):
        for f in range(0, wg_ref.shape[1], cut):
            at = slice(f, f + cut)
            gate, up = dot(b, wg_ref[:, at]), dot(b, wu_ref[:, at])
            gate_ref[part, at] = gate
            up_ref[part, at] = up
            s_s[part, at] = low(gated(gate, up))
        h3 = low(wide(h) + wide(low(dot(s_s[part, :], wd_ref[:]))))
        h3_ref[part, :] = h3
        h = wide(h3)
        project(part, low(h * root(h)), wq_ref[:], w_kv[:], cos_ref, sin_ref, q_ref, k_ref, v_ref)


def mid(h, o, tables, w, number, bt=512, cut=512, size=256):
    tokens, d = h.shape
    wq, wk, wv, wo, wg, wu, wd = (w[name] for name in NAMES)
    dk, ff = wk.shape[2], wg.shape[2]
    return pl.pallas_call(
        functools.partial(_mid, cut=cut, size=size),
        grid=(tokens // bt,),
        in_specs=[rows(bt, d), rows(bt, d)] + [rows(bt, HEAD)] * 2 + [one_layer(a, number) for a in (wo, wg, wu, wd)]
        + [one_layer(a, number + 1) for a in (wq, wk, wv)],
        out_specs=[rows(bt, d), rows(bt, ff), rows(bt, ff), rows(bt, d), rows(bt, wq.shape[2]), rows(bt, dk), rows(bt, dk)],
        out_shape=[like(tokens, d), like(tokens, ff, jnp.float32), like(tokens, ff, jnp.float32), like(tokens, d),
                   like(tokens, wq.shape[2]), like(tokens, dk), like(tokens, dk)],
        scratch_shapes=[pltpu.VMEM((d, 2 * dk), jnp.bfloat16), pltpu.VMEM((bt, ff), jnp.bfloat16)],
        compiler_params=params(),
        name="mid",
    )(h, o, *tables, wo, wg, wu, wd, wq, wk, wv)


def _tail(h_ref, o_ref, dy_ref, *rest, blocks, cut, out, size, saved):
    if saved:
        gate_ref, up_ref, *rest = rest
    (wo_ref, wg_ref, wu_ref, wd_ref, dh2_ref, do_ref, delta_ref, gg_ref, gu_ref, gd_ref, go_ref,
     b_t, dy_t, s_s, dgate_s, dup_s, go_s) = rest
    i = pl.program_id(0)
    bt, d = dy_ref.shape
    ff = wg_ref.shape[1]

    @pl.when(i == 0)
    def _():
        go_s[:] = jnp.zeros_like(go_s)

    @pl.when(i < blocks)
    def _():
        own = lax.div(lax.broadcasted_iota(jnp.int32, (8, d), 1), HEAD) == lax.broadcasted_iota(jnp.int32, (8, d), 0)
        pick = jnp.where(own, 1.0, 0.0).astype(jnp.bfloat16)
        state = []
        for part in parts_of(bt, size):
            h = wide(h_ref[part, :])
            if not saved:
                h = wide(low(h + wide(low(dot(o_ref[part, :], wo_ref[:])))))
            r = root(h)
            state.append((part, pl.ds(pl.multiple_of(i * bt + part.start, size), size), low(h), r, low(h * r)))
        for part, here, h, r, b in state:
            dy, o = dy_ref[part, :], o_ref[part, :]
            by_b = jnp.zeros((size, d), jnp.float32)
            for f in range(0, ff, cut):
                at = slice(f, f + cut)
                if saved:
                    gate, up = gate_ref[part, at], up_ref[part, at]
                else:
                    gate, up = dot(b, wg_ref[:, at]), dot(b, wu_ref[:, at])
                by_s = dot_t(dy, wd_ref[at, :])
                sig = jax.nn.sigmoid(gate)
                act = gate * sig
                s_s[here, at] = low(act * up)
                dup = low(by_s * act)
                dgate = low(by_s * up * (sig + act * (1 - sig)))
                dup_s[here, at] = dup
                dgate_s[here, at] = dgate
                by_b += dot_t(dgate, wg_ref[:, at]) + dot_t(dup, wu_ref[:, at])
            dh2 = low(wide(dy) + norm_back(wide(h), r, by_b))
            dh2_ref[part, :] = dh2
            do = low(dot_t(dh2, wo_ref[:]))
            do_ref[part, :] = do
            both = wide(do) * wide(o)
            first = low(both)
            second = low(both - wide(first))
            delta_ref[:, part] = dot_t(pick, first) + dot_t(pick, second)
            go_s[:] += dot(o.T, dh2)
            b_t[:, here] = b.T
            dy_t[:, here] = dy.T

    @pl.when(i >= blocks)
    def _():
        at = pl.ds(pl.multiple_of((i - blocks) * out, out), out)
        gg_ref[:] = low(dot(b_t[:], dgate_s[:, at]))
        gu_ref[:] = low(dot(b_t[:], dup_s[:, at]))
        gd_ref[:] = low(dot(dy_t[:], s_s[:, at]).T)

    @pl.when(i == pl.num_programs(0) - 1)
    def _():
        go_ref[:] = low(go_s[:])


def tail(h, o, dy, w, number, kept=None, bt=256, cut=512, out=256):
    tokens, d = dy.shape
    wo, wg, wu, wd = (w[name] for name in NAMES[3:])
    ff = wg.shape[2]
    blocks, last = tokens // bt, tokens // bt - 1
    after = lambda i: jnp.maximum(i - blocks, 0)
    return pl.pallas_call(
        functools.partial(_tail, blocks=blocks, cut=cut, out=out, size=256, saved=kept is not None),
        grid=(blocks + ff // out,),
        in_specs=[rows(bt, d, last)] * 3 + ([] if kept is None else [rows(bt, ff, last)] * 2) + [one_layer(a, number) for a in (wo, wg, wu, wd)],
        out_specs=[rows(bt, d, last), rows(bt, d, last), pl.BlockSpec((8, bt), lambda i: (0, jnp.minimum(i, last))),
                   pl.BlockSpec((d, out), lambda i: (0, after(i))), pl.BlockSpec((d, out), lambda i: (0, after(i))),
                   pl.BlockSpec((out, d), lambda i: (after(i), 0)), whole((d, d), pipeline_mode=pl.Buffered(1))],
        out_shape=[like(tokens, d), like(tokens, d), like(8, tokens, jnp.float32), like(d, ff), like(d, ff), like(ff, d), like(d, d)],
        scratch_shapes=[pltpu.VMEM((d, tokens), jnp.bfloat16)] * 2 + [pltpu.VMEM((tokens, ff), jnp.bfloat16)] * 3 + [pltpu.VMEM((d, d), jnp.float32)],
        compiler_params=params(),
        name="tail",
    )(h, o, dy, *(kept or ()), wo, wg, wu, wd)


def turned_back(dq_ref, dk_ref, dv_ref, cos, sin, d_s, here):
    width = dq_ref.shape[1]
    for at in heads_of(width):
        d_s[here, at] = low(turned(wide(dq_ref[:, at]), cos, sin, -1))
    d_s[here, width : width + HEAD] = low(turned(wide(dk_ref[:]), cos, sin, -1))
    d_s[here, width + HEAD :] = dv_ref[:]


def _back(h_ref, dh2_ref, dq_ref, dk_ref, dv_ref, cos_ref, sin_ref, wq_ref, wk_ref, wv_ref, dh_ref, gq_ref, gk_ref, gv_ref, a_t, d_s, w_kv, *, blocks):
    i = pl.program_id(0)

    @pl.when(i == 0)
    def _():
        w_kv[:, :HEAD] = wk_ref[:]
        w_kv[:, HEAD:] = wv_ref[:]

    bt, d = h_ref.shape
    dq_w = dq_ref.shape[1]
    here = pl.ds(pl.multiple_of(i * bt, bt), bt)
    h = wide(h_ref[:])
    r = root(h)
    a_t[:, here] = low(h * r).T
    turned_back(dq_ref, dk_ref, dv_ref, cos_ref[:], sin_ref[:], d_s, here)
    by_a = dot_t(d_s[here, :dq_w], wq_ref[:]) + dot_t(d_s[here, dq_w:], w_kv[:])
    dh_ref[:] = low(wide(dh2_ref[:]) + norm_back(h, r, by_a))

    @pl.when(i == blocks - 1)
    def _():
        got = low(dot(a_t[:], d_s[:]))
        gq_ref[:] = got[:, :dq_w]
        gk_ref[:] = got[:, dq_w : dq_w + HEAD]
        gv_ref[:] = got[:, dq_w + HEAD :]


def back(h, dh2, dq, dk, dv, tables, w, number, bt=512):
    tokens, d = h.shape
    wq, wk, wv = (w[name] for name in NAMES[:3])
    blocks = tokens // bt
    return pl.pallas_call(
        functools.partial(_back, blocks=blocks),
        grid=(blocks,),
        in_specs=[rows(bt, d), rows(bt, d), rows(bt, dq.shape[1]), rows(bt, HEAD), rows(bt, HEAD), rows(bt, HEAD), rows(bt, HEAD)]
        + [one_layer(a, number) for a in (wq, wk, wv)],
        out_specs=[rows(bt, d)] + [whole(a.shape[1:]) for a in (wq, wk, wv)],
        out_shape=[like(tokens, d)] + [like(*a.shape[1:]) for a in (wq, wk, wv)],
        scratch_shapes=[pltpu.VMEM((d, tokens), jnp.bfloat16), pltpu.VMEM((tokens, dq.shape[1] + 2 * HEAD), jnp.bfloat16), pltpu.VMEM((d, 2 * HEAD), jnp.bfloat16)],
        compiler_params=params(),
        name="back",
    )(h, dh2, dq, dk, dv, *tables, wq, wk, wv)


def tables_of(tokens, stride=64):
    half = HEAD // 2
    speed = THETA ** (-jnp.arange(half, dtype=jnp.float32) / half)

    def both(places):
        angle = places.astype(jnp.float32)[:, None] * speed
        return jnp.cos(angle), jnp.sin(angle)

    (c1, s1), (c2, s2) = both(jnp.arange(0, tokens, stride)), both(jnp.arange(stride))
    (c1, s1), (c2, s2) = (c1[:, None], s1[:, None]), (c2[None], s2[None])
    cos, sin = ((c1 * c2 - s1 * s2).reshape(tokens, half), (s1 * c2 + c1 * s2).reshape(tokens, half))
    return jnp.concatenate([cos, cos], 1), jnp.concatenate([-sin, sin], 1)


CORES = 2


class Place:
    def __init__(self, n):
        self.n = n
        self.side = side = math.isqrt(n // CORES)
        self.me = me = lax.axis_index("dp")
        self.core = lax.rem(me, CORES)
        self.y = lax.rem(lax.div(me, CORES), side)
        self.x = lax.div(me, CORES * side)
        self.twin = me + 1 - 2 * self.core

    def at(self, axis):
        return self.x if axis == 0 else self.y

    def along(self, axis, by):
        if axis == 0:
            return lax.rem(self.x + by + self.side, self.side) * (CORES * self.side) + self.y * CORES + self.core
        return self.x * (CORES * self.side) + lax.rem(self.y + by + self.side, self.side) * CORES + self.core

    def near(self):
        return [self.twin] + [self.along(axis, by) for axis in (0, 1) for by in (1, -1)]


def greet(devices):
    for d in devices:
        pl.semaphore_signal(pltpu.get_barrier_semaphore(), inc=1, device_id={"dp": d}, device_id_type=pl.DeviceIdType.MESH)


def greeted(count):
    pl.semaphore_wait(pltpu.get_barrier_semaphore(), count)


def greet_all(place):
    barrier = pltpu.get_barrier_semaphore()

    def hello(k, _):
        pl.semaphore_signal(barrier, inc=1, device_id={"dp": lax.rem(place.me + k, place.n)}, device_id_type=pl.DeviceIdType.MESH)

    lax.fori_loop(1, place.n, hello, None)


def send(src, dst, sems, device):
    return pltpu.make_async_remote_copy(src, dst, sems[0], sems[1], device_id={"dp": device}, device_id_type=pl.DeviceIdType.MESH)


class Scatter:
    def __init__(self, place, pieces, g_refs, buffers, sems, out_refs):
        self.p, self.pieces, self.g_refs, self.out_refs = place, pieces, g_refs, out_refs
        self.buffers = [buffers[4 * i : 4 * i + 4] for i in range(len(pieces))]
        self.send_s, self.recv_s, self.local_s = sems
        self.half = place.side // 2

    @staticmethod
    def scratch(pieces, side):
        out, half = [], side // 2
        for _, r, c, *_ in pieces:
            r, c = r.stop - r.start, c.stop - c.start
            out += [pltpu.VMEM((side, side, r, c), jnp.bfloat16), pltpu.VMEM((side, side, r, c), jnp.bfloat16),
                    pltpu.VMEM((half, 2, side, r, c), jnp.bfloat16), pltpu.VMEM((half, 2, r, c), jnp.bfloat16)]
        count = len(pieces)
        return out, [pltpu.SemaphoreType.DMA((count, 1 + 4 * half)), pltpu.SemaphoreType.DMA((count, 1 + 4 * half)), pltpu.SemaphoreType.DMA((count,))]

    def pair(self, i, k):
        return self.send_s.at[i, k], self.recv_s.at[i, k]

    def twin_copies(self, i):
        g, r, c, *_ = self.pieces[i]
        g, (own, came, _, _), p = self.g_refs[g], self.buffers[i], self.p
        return (send(g.at[:, :, 1 - p.core, r, c], came, self.pair(i, 0), p.twin),
                pltpu.make_async_copy(g.at[:, :, p.core, r, c], own, self.local_s.at[i]))

    def start(self, i):
        for c in self.twin_copies(i):
            c.start()

    def join_twin(self, i):
        own, came, _, _ = self.buffers[i]
        far, near = self.twin_copies(i)
        near.wait()
        far.wait()

        def add(k, _):
            own[k] = low(wide(own[k]) + wide(came[k]))

        lax.fori_loop(0, self.p.side, add, None)

    def moves(self, i, stage, t):
        first = self.pieces[i][3]
        own, _, across, last = self.buffers[i]
        p, half = self.p, self.half
        axis = first if stage == 0 else 1 - first
        away = half - t
        cols = own.shape[3]
        out = []
        for way, by in enumerate((1, -1)):
            to = lax.rem(p.at(axis) + by * away + p.side, p.side)
            into = lax.rem(p.at(axis) + by * (away - 1) + p.side, p.side)
            if stage == 0:
                part = pl.ds(way * half, half) if away == half else pl.ds(0, p.side)
                view = lambda k: own.at[k, part] if axis == 0 else own.at[part, k]
                arrived = across.at[t, way, pl.ds(0, part.size)]
            else:
                if away < half:
                    part = pl.ds(0, cols)
                elif cols >= 256:
                    middle = cols // 256 * 128
                    part = pl.ds(0, middle) if way == 0 else pl.ds(middle, cols - middle)
                elif way == 0:
                    part = pl.ds(0, cols)
                else:
                    continue
                view = lambda k: own.at[k, p.y, :, part] if axis == 0 else own.at[p.x, k, :, part]
                arrived = last.at[t, way, :, pl.ds(0, part.size)]
            copy = send(view(to), arrived, self.pair(i, 1 + 2 * half * stage + 2 * t + way), p.along(axis, by))
            out.append((copy, view(into), arrived))
        return out

    def hop(self, i, stage, t):
        for copy, _, _ in self.moves(i, stage, t):
            copy.start()

    def join(self, i, stage, t):
        moves = self.moves(i, stage, t)
        for copy, _, _ in moves:
            copy.wait()
        if t == self.half - 1 and self.half > 1:
            moves = [(moves[0][1], [arrived for _, _, arrived in moves])]
        else:
            moves = [(into, [arrived]) for _, into, arrived in moves]
        for into, arrived in moves:
            total = wide(into[:])
            for a in arrived:
                total += wide(a[:])
            into[:] = low(total)

    def phase(self, k, group, squares):
        for i in group:
            if k == 0:
                self.start(i)
            elif k == 1:
                self.join_twin(i)
                self.hop(i, 0, 0)
            else:
                stage, t = (k - 2) // self.half, (k - 2) % self.half
                self.join(i, stage, t)
                if k < 1 + 2 * self.half:
                    self.hop(i, (k - 1) // self.half, (k - 1) % self.half)
                else:
                    done = self.buffers[i][0][self.p.x, self.p.y]
                    self.out_refs[i][:] = done
                    squares[:] += sum_tiles(wide(done) * wide(done))

    @property
    def last(self):
        return 1 + 2 * self.half


def pieces_of(names, shapes, n):
    out = []
    for g, (name, (rows, cols)) in enumerate(zip(names, shapes)):
        r, c, middle = slice(0, rows // n), slice(0, cols), cols // 2
        halves = [slice(0, middle), slice(middle, cols)]
        if name in ("w_gate", "w_up"):
            out += [(g, r, part, int(name == "w_up"), group) for group, part in enumerate(halves)]
        elif name == "w_down":
            out += [(g, part, c, axis, 2) for axis, part in enumerate((slice(0, r.stop // 2), slice(r.stop // 2, r.stop)))]
        elif cols > HEAD:
            out += [(g, r, part, axis, 3) for axis, part in enumerate(halves)]
        else:
            out.append((g, r, c, int(name == "wv"), 3))
    return out


def blocked(g, n):
    side = math.isqrt(n // CORES)
    return g.reshape(side, side, CORES, g.shape[0] // n, g.shape[1])


def piece_shape(piece):
    return jax.ShapeDtypeStruct((piece[1].stop - piece[1].start, piece[2].stop - piece[2].start), jnp.bfloat16)


def sum_tiles(wide):
    rows, cols = wide.shape
    out = jnp.zeros((8, 128), jnp.float32)
    for a in range(0, rows, 8):
        for b in range(0, cols, 128):
            out = out + wide[a : a + 8, b : b + 128]
    return out


def everyone(place, part, slots, send_s, recv_s, total_ref):
    slots[place.me] = part[:]

    def copy(k):
        return send(part, slots.at[place.me], (send_s.at[k], recv_s), lax.rem(place.me + k, place.n))

    lax.fori_loop(1, place.n, lambda k, _: copy(k).start(), None)
    lax.fori_loop(1, place.n, lambda k, _: copy(k).wait_send(), None)
    pltpu.make_async_copy(slots.at[pl.ds(0, place.n - 1)], slots.at[pl.ds(0, place.n - 1)], recv_s).wait()
    total_ref[:] = lax.fori_loop(0, place.n, lambda k, so_far: so_far + slots[k], jnp.zeros_like(part))


STREAMS = ((0, 1), (0, -1), (1, 1), (1, -1))


def stream_of(name, number):
    return {"w_up": 2, "w_down": 3}.get(name, number % 2)


def settled(arrays):
    count = len(arrays)

    def kernel(*refs):
        sems = refs[2 * count]
        copies = [pltpu.make_async_copy(refs[i], refs[count + i], sems.at[i]) for i in range(count)]
        for c in copies:
            c.start()
        for c in copies:
            c.wait()

    return pl.pallas_call(
        kernel,
        in_specs=[pl.BlockSpec(memory_space=pltpu.VMEM)] * count,
        out_specs=[pl.BlockSpec(memory_space=pltpu.HBM)] * count,
        out_shape=[jax.ShapeDtypeStruct(a.shape, a.dtype) for a in arrays],
        scratch_shapes=[pltpu.SemaphoreType.DMA((count,))],
        compiler_params=pltpu.CompilerParams(vmem_limit_bytes=SMALL),
        name="settle",
    )(*arrays)


def gathered(shards, n):
    side = math.isqrt(n // CORES)
    names = list(shards)
    steps = side - 1
    layers = shards[names[0]].shape[0]
    pieces = []
    for i, name in enumerate(names):
        pieces += [(i, k, k + 1, stream_of(name, k)) for k in range(layers)]
    count, legs = len(pieces), steps + side * steps

    def kernel(*refs):
        mine, outs = refs[: len(names)], refs[len(names) : 2 * len(names)]
        send_s, recv_s, twin_send, twin_recv, local_s = refs[2 * len(names) :]
        place = Place(n)
        greet(place.near())
        greeted(len(place.near()))

        def block(i, ref, p1, p2):
            array, a, b, stream = pieces[i]
            x, y = (p1, p2) if STREAMS[stream][0] == 0 else (p2, p1)
            return ref.at[pl.ds(a, b - a), x, y, place.core]

        def own(i):
            array, a, b, _ = pieces[i]
            return mine[array].at[pl.ds(a, b - a)]

        def spot(i, back1, back2):
            first, by = STREAMS[pieces[i][3]]
            return tuple(lax.rem(place.at(axis) - by * back + 2 * side, side) for axis, back in ((first, back1), (1 - first, back2)))

        def hop(i, leg, stage, back1, back2):
            first, by = STREAMS[pieces[i][3]]
            axis = first if stage == 0 else 1 - first
            out = outs[pieces[i][0]]
            at = block(i, out, *spot(i, back1, back2))
            return send(own(i) if back1 == back2 == 0 else at, at, (send_s.at[i, leg], recv_s.at[i, leg]), place.along(axis, by))

        def to_twin(i, k, back1, back2):
            at = block(i, outs[pieces[i][0]], *spot(i, back1, back2))
            return send(own(i) if back1 == back2 == 0 else at, at, (twin_send.at[i, k], twin_recv.at[i, k]), place.twin)

        def first_leg(t):
            return t

        def second_leg(j, t):
            return steps + j * steps + t

        started = []

        def go(copy):
            copy.start()
            started.append(copy)

        keep = [pltpu.make_async_copy(own(i), block(i, outs[pieces[i][0]], *spot(i, 0, 0)), local_s.at[i]) for i in range(count)]
        for i in range(count):
            go(hop(i, first_leg(0), 0, 0, 0))
            go(hop(i, second_leg(0, 0), 1, 0, 0))
        for i in range(count):
            keep[i].start()
            go(to_twin(i, 0, 0, 0))
        for k in range(2 * steps):
            for i in range(count):
                if k < steps:
                    hop(i, first_leg(k), 0, k, 0).wait_recv()
                    if k + 1 < steps:
                        go(hop(i, first_leg(k + 1), 0, k + 1, 0))
                    go(hop(i, second_leg(k + 1, 0), 1, k + 1, 0))
                    go(to_twin(i, (k + 1) * side, k + 1, 0))
                for j in range(side):
                    t = k - j
                    if 0 <= t < steps:
                        hop(i, second_leg(j, t), 1, j, t).wait_recv()
                        if t + 1 < steps:
                            go(hop(i, second_leg(j, t + 1), 1, j, t + 1))
                        go(to_twin(i, j * side + t + 1, j, t + 1))
        for i in range(count):
            keep[i].wait()
            for back1 in range(side):
                for back2 in range(side):
                    to_twin(i, back1 * side + back2, back1, back2).wait_recv()
        for copy in started:
            copy.wait_send()

    vmem = pl.BlockSpec(memory_space=pltpu.VMEM)
    outs = pl.pallas_call(
        kernel,
        in_specs=[vmem] * len(names),
        out_specs=[vmem] * len(names),
        out_shape=[pltpu.VMEM((layers, side, side, CORES, *s.shape[1:]), s.dtype) for s in shards.values()],
        scratch_shapes=[pltpu.SemaphoreType.DMA((count, legs)), pltpu.SemaphoreType.DMA((count, legs)),
                        pltpu.SemaphoreType.DMA((count, side * side)), pltpu.SemaphoreType.DMA((count, side * side)), pltpu.SemaphoreType.DMA((count,))],
        compiler_params=pltpu.CompilerParams(collective_id=1, has_side_effects=True, vmem_limit_bytes=SMALL),
        name="gather",
    )(*shards.values())
    return settled([out.reshape(layers, -1, out.shape[-1]) for out in outs])


def stepped(pieces, total, weights, m, v, n, count):
    arrays = len(weights)

    def kernel(me_ref, total_ref, *refs):
        g_refs, refs = refs[: len(pieces)], refs[len(pieces) :]
        w_refs, m_refs, v_refs, w_out, m_out, v_out = (refs[arrays * k : arrays * (k + 1)] for k in range(6))
        squares = jnp.sum(total_ref[:], keepdims=True)
        factor = jnp.minimum(1.0, 0.5 * lax.rsqrt(squares / count + 1e-30))
        for (i, k, r, c, _), g_ref in zip(pieces, g_refs):
            g = wide(g_ref[:]) * factor
            new_m = 0.9 * m_refs[i][k, r, c] + 0.1 * g
            new_v = 0.95 * v_refs[i][k, r, c] + 0.05 * g * g
            w = wide(w_refs[i][k, 0, r, c])
            step = new_m * lax.rsqrt(new_v + 1e-8) + 0.1 * w
            w_out[i][k, r, c] = low(w - 0.02 * step)
            m_out[i][k, r, c] = new_m
            v_out[i][k, r, c] = new_v

    own = lambda a: pl.BlockSpec((a.shape[0], 1, a.shape[1] // n, a.shape[2]), lambda i, me: (0, me[0], 0, 0))
    flat = [g for *_, g in pieces]
    out = pl.pallas_call(
        kernel,
        grid_spec=pltpu.PrefetchScalarGridSpec(
            num_scalar_prefetch=1,
            grid=(1,),
            in_specs=[whole(total.shape)] + [whole(g.shape) for g in flat] + [own(w) for w in weights] + [whole(a.shape) for a in (*m, *v)],
            out_specs=[pl.BlockSpec(memory_space=pltpu.VMEM)] * arrays + [whole(a.shape) for a in (*m, *v)],
        ),
        out_shape=[pltpu.VMEM(a.shape, jnp.bfloat16) for a in m] + [jax.ShapeDtypeStruct(a.shape, a.dtype) for a in (*m, *v)],
        compiler_params=pltpu.CompilerParams(vmem_limit_bytes=VMEM),
        name="adamw",
    )(lax.axis_index("dp").reshape(1), total, *flat, *(w.reshape(w.shape[0], n, -1, w.shape[2]) for w in weights), *m, *v)
    return out[:arrays], out[arrays : 2 * arrays], out[2 * arrays :]


def cut_off(keys, queries, ahead=0):
    return lax.broadcasted_iota(jnp.int32, (keys, queries), 1) >= lax.broadcasted_iota(jnp.int32, (keys, queries), 0) + ahead


def _forward(q_ref, k_ref, v_ref, o_ref, lse_ref, base_s, mix_s, *, part, e):
    bq, width = q_ref.shape
    heads = heads_of(width)
    iq = pl.program_id(0)

    def values(here, count):
        return jnp.concatenate([v_ref[here, :].T, jnp.ones((8, count), jnp.bfloat16)], axis=0)

    def block(at, count, seen, masked):
        here = pl.ds(pl.multiple_of(at, count), count)
        k, mixed = k_ref[here, :], values(here, count)
        score = lambda n: dot_t(k, q_ref[seen:, heads[n]])

        def weight(n, s):
            p = jnp.exp2(s * e - base_s[n : n + 1, seen:])
            return low(jnp.where(cut_off(count, bq - seen), p, 0.0) if masked else p)

        last = len(heads) - 1
        s, p = score(0), None
        for n in range(last + 2):
            following = score(n + 1) if n < last else None
            new = weight(n, s) if n <= last else None
            if n > 0:
                mix_s[n - 1, :, seen:] += dot(mixed, p)
            s, p = following, new

    for n, head in enumerate(heads):
        base_s[n : n + 1, :] = dot_t(k_ref[:8, :], q_ref[:, head])[:1] * e
    mix_s[:] = jnp.zeros_like(mix_s)
    lax.fori_loop(0, iq, lambda j, _: block(j * bq, bq, 0, False), None)
    for at in range(0, bq, part):
        block(iq * bq + at, part, at, True)

    @pl.when(jnp.sum(jnp.where(jnp.abs(mix_s[:]) < BIG, 0.0, 1.0)) > 0)
    def _():
        def again(j, n):
            here = pl.ds(pl.multiple_of(j * bq, bq), bq)
            head = pl.ds(pl.multiple_of(n * HEAD, HEAD), HEAD)
            s = jnp.where(cut_off(bq, bq, (j - iq) * bq), dot_t(k_ref[here, :], q_ref[:, head]) * e, 2 * NEG)
            old = base_s[pl.ds(n, 1), :]
            top = jnp.maximum(old, s.max(axis=0, keepdims=True))
            base_s[pl.ds(n, 1), :] = top
            mix_s[n] = mix_s[n] * jnp.exp2(old - top) + dot(values(here, bq), low(jnp.exp2(s - top)))
            return n

        base_s[:] = jnp.full_like(base_s, NEG)
        mix_s[:] = jnp.zeros_like(mix_s)
        lax.fori_loop(0, len(heads), lambda n, _: lax.fori_loop(0, iq + 1, again, n), 0)

    for n, head in enumerate(heads):
        total = mix_s[n, HEAD : HEAD + 1, :]
        o_ref[:, head] = low((mix_s[n, :HEAD, :] * (1 / total)).T)
        lse_ref[n : n + 1, :] = base_s[n : n + 1, :] + jnp.log(total) * LOG2E


def attend(q, k, v, bq=1024, part=256):
    tokens, width = q.shape
    heads = width // HEAD
    every_key = whole((tokens, HEAD))
    return pl.pallas_call(
        functools.partial(_forward, part=part, e=HEAD**-0.5 * LOG2E),
        grid=(tokens // bq,),
        in_specs=[rows(bq, width), every_key, every_key],
        out_specs=[rows(bq, width), pl.BlockSpec((8, bq), lambda i: (0, i))],
        out_shape=[like(tokens, width), like(8, tokens, jnp.float32)],
        scratch_shapes=[pltpu.VMEM((8, bq), jnp.float32), pltpu.VMEM((heads, HEAD + 8, bq), jnp.float32)],
        compiler_params=params(),
        name="attend",
    )(q, k, v)


SLOTS = 3
WHEN = ((3, 5, 8, 12, 18, 24), (3, 6, 9, 16, 21, 25), (3, 8, 13, 20, 24, 26), (3, 9, 17, 23, 25, 27))


def attend_back(q, k, v, do, lse, delta, terms, n, number, bq=512, part=256):
    tokens, width = q.shape
    heads, e = heads_of(width), HEAD**-0.5 * LOG2E
    blocks, scale = tokens // bq, HEAD**-0.5
    steps = blocks * (blocks + 1) // 2
    side = math.isqrt(n // CORES)
    pieces = pieces_of([name for name, _, _ in terms], [g.shape for _, _, g in terms], n)
    count = len(pieces)
    buffers, sems = Scatter.scratch(pieces, side)
    groups = [[i for i, p in enumerate(pieces) if p[4] == group] for group in range(4)]

    def block_of(i):
        return sum(jnp.where(i >= row * (row + 1) // 2, 1, 0) for row in range(1, blocks))

    def kernel(q_ref, k_ref, v_ref, do_ref, lse_ref, delta_ref, *refs):
        g_refs, (dq_ref, dk_ref, dv_ref, *refs) = refs[: len(terms)], refs[len(terms) :]
        out_refs, squares_ref, (dq_s, dk_s, dv_s, *refs) = refs[:count], refs[count], refs[count + 1 :]
        i = pl.program_id(0)
        iq = block_of(i)
        j = i - lax.div(iq * (iq + 1), 2)
        place = Place(n)
        rs = Scatter(place, pieces, g_refs, refs[: len(buffers)], refs[len(buffers) :], out_refs)

        @pl.when(i == 0)
        def _():
            greet(place.near())
            dk_s[:] = jnp.zeros_like(dk_s)
            dv_s[:] = jnp.zeros_like(dv_s)
            squares_ref[:] = jnp.zeros_like(squares_ref)

        def beside(steps_here, slots):
            for at in steps_here:
                todo = [(phase, group) for group, times in zip(groups, WHEN) for phase, time in enumerate(times)
                        if time // SLOTS == at and time % SLOTS in slots]
                if todo:
                    @pl.when(i == at)
                    def _():
                        for phase, group in todo:
                            rs.phase(phase, group, squares_ref)

        @pl.when(i == 1)
        def _():
            greeted(len(place.near()))

        beside(range(steps), (0,))

        @pl.when(j == 0)
        def _():
            dq_s[:] = jnp.zeros_like(dq_s)

        def block(at, size, seen, masked, some):
            here = pl.ds(pl.multiple_of(at, size), size)
            k, v = k_ref[here, :], v_ref[here, :]
            k_t = k.T
            ok = cut_off(size, bq - seen) if masked else None
            scores = [dot_t(k, q_ref[seen:, head]) for _, head in some]
            dps = [dot_t(v, do_ref[seen:, head]) for _, head in some]
            for (n, head), s, dp in zip(some, scores, dps):
                p = jnp.exp2(s * e - lse_ref[n : n + 1, seen:])
                if masked:
                    p = jnp.where(ok, p, 0.0)
                ds = low(p * (dp - delta_ref[n : n + 1, seen:]))
                dv_s[here, :] += dot(low(p), do_ref[seen:, head])
                dk_s[here, :] += dot(ds, q_ref[seen:, head])
                dq_s[n, :, seen:] += dot(k_t, ds)

        every = list(enumerate(heads))
        ends = [row * (row + 3) // 2 for row in range(blocks)]

        @pl.when(j < iq)
        def _():
            share = len(every) // SLOTS
            for slot in range(SLOTS):
                if slot:
                    beside([at for at in range(steps) if at not in ends], (slot,))
                block(j * bq, bq, 0, False, every[slot * share : (slot + 1) * share])

        @pl.when(j == iq)
        def _():
            block(j * bq, part, 0, True, every)
            beside(ends, range(1, SLOTS))
            for seen in range(part, bq, part):
                block(j * bq + seen, part, seen, True, every)
            for n, head in every:
                dq_ref[:, head] = low((dq_s[n] * scale).T)

        @pl.when(i == steps - 1)
        def _():
            for phase in range(rs.last + 1):
                for group, times in zip(groups, WHEN):
                    if times[phase] >= SLOTS * steps:
                        rs.phase(phase, group, squares_ref)
            dk_ref[:] = low(dk_s[:] * scale)
            dv_ref[:] = low(dv_s[:])

    every_key = whole((tokens, HEAD))
    mine = pl.BlockSpec((bq, width), lambda i: (block_of(i), 0))
    stats = pl.BlockSpec((8, bq), lambda i: (0, block_of(i)))
    sums = [piece_shape(p) for p in pieces] + [like(8, HEAD, jnp.float32)]
    dq, dk, dv, *outs = pl.pallas_call(
        kernel,
        grid=(steps,),
        in_specs=[mine, every_key, every_key, mine, stats, stats] + [pl.BlockSpec(memory_space=pl.ANY)] * len(terms),
        out_specs=[mine, every_key, every_key] + [whole(s.shape) for s in sums],
        out_shape=[like(tokens, width), like(tokens, HEAD), like(tokens, HEAD)] + sums,
        scratch_shapes=[pltpu.VMEM((len(heads), HEAD, bq), jnp.float32), pltpu.VMEM((tokens, HEAD), jnp.float32), pltpu.VMEM((tokens, HEAD), jnp.float32)]
        + buffers + sems,
        compiler_params=pltpu.CompilerParams(dimension_semantics=("arbitrary",), vmem_limit_bytes=MOST, collective_id=2 + number, has_side_effects=True),
        name="attend_back",
    )(q, k, v, do, lse, delta, *(blocked(g, n) for _, _, g in terms))
    return dq, dk, dv, list(zip(pieces, outs)), outs[count]


def finished(h, dq, dk, dv, tables, w, number, squares, n, bt=512):
    tokens, d = h.shape
    names = NAMES[:3]
    widths = [w[name].shape[-1] for name in names]
    blocks, side = tokens // bt, math.isqrt(n // CORES)
    pieces = pieces_of(names, [(d, c) for c in widths], n)
    count = len(pieces)
    buffers, sems = Scatter.scratch(pieces, side)

    def kernel(h_ref, dq_ref, dk_ref, dv_ref, cos_ref, sin_ref, *refs):
        squares_refs, refs = refs[: len(squares)], refs[len(squares) :]
        out_refs, total_ref, a_t, d_s, *refs = refs[:count], refs[count], *refs[count + 1 :]
        g_refs, refs = refs[: len(names)], refs[len(names) :]
        own, (send_s, recv_s, local_s, part, slots, sq_send, sq_recv) = refs[: len(buffers)], refs[len(buffers) :]
        i = pl.program_id(0)
        place = Place(n)

        @pl.when(i == 0)
        def _():
            greet_all(place)

        here = pl.ds(pl.multiple_of(i * bt, bt), bt)
        h = wide(h_ref[:])
        a_t[:, here] = low(h * root(h)).T
        turned_back(dq_ref, dk_ref, dv_ref, cos_ref[:], sin_ref[:], d_s, here)

        @pl.when(i == blocks - 1)
        def _():
            homes = [(g_ref, slice(at, at + HEAD)) for g_ref, width in zip(g_refs, widths) for at in range(0, width, HEAD)]
            for k in range(0, len(homes), 2):
                got = low(dot(a_t[:], d_s[:, k * HEAD : (k + 2) * HEAD]).reshape(side, side, CORES, -1, 2 * HEAD))
                for (g_ref, at), mine in zip(homes[k : k + 2], (got[..., :HEAD], got[..., HEAD:])):
                    g_ref[:, :, :, :, at] = mine
            greeted(place.n - 1)
            rs = Scatter(place, pieces, g_refs, own, (send_s, recv_s, local_s), out_refs)
            part[:] = sum(ref[:] for ref in squares_refs)
            for k in range(rs.last + 1):
                rs.phase(k, range(count), part)
            everyone(place, part, slots, sq_send, sq_recv, total_ref)

    sums = [piece_shape(p) for p in pieces] + [like(8, HEAD, jnp.float32)]
    outs = pl.pallas_call(
        kernel,
        grid=(blocks,),
        in_specs=[rows(bt, d), rows(bt, dq.shape[1])] + [rows(bt, HEAD)] * 4 + [whole(s.shape) for s in squares],
        out_specs=[whole(s.shape) for s in sums],
        out_shape=sums,
        scratch_shapes=[pltpu.VMEM((d, tokens), jnp.bfloat16), pltpu.VMEM((tokens, sum(widths)), jnp.bfloat16)]
        + [pltpu.VMEM((side, side, CORES, d // n, c), jnp.bfloat16) for c in widths] + buffers + sems
        + [pltpu.VMEM((8, HEAD), jnp.float32), pltpu.VMEM((n, 8, HEAD), jnp.float32), pltpu.SemaphoreType.DMA((n,)), pltpu.SemaphoreType.DMA],
        compiler_params=pltpu.CompilerParams(dimension_semantics=("arbitrary",), collective_id=0, has_side_effects=True, vmem_limit_bytes=VMEM),
        name="finish",
    )(h, dq, dk, dv, *tables, *squares)
    return list(zip(pieces, outs)), outs[count]


def summed(x, dy, w, n):
    tables = tables_of(x.shape[0])
    layers = w["wq"].shape[0]
    h, kept = x, []
    q, k, v = pre(h, tables, w, 0)
    for number in range(layers):
        o, lse = attend(q, k, v)
        if number < layers - 1:
            h2, gate, up, h3, *following = mid(h, o, tables, w, number)
            kept.append((h, q, k, v, o, lse, h2, (gate, up)))
            h, (q, k, v) = h3, following
        else:
            kept.append((h, q, k, v, o, lse, h, None))
    by_h, waiting, sums, squares = dy, [], [], []

    def note(terms, got):
        for (g, r, c, *_), block in got:
            sums.append((NAMES.index(terms[g][0]), terms[g][1], r, c, block))

    for number in reversed(range(layers)):
        h, q, k, v, o, lse, between, saved = kept[number]
        dh2, do, delta, gg, gu, gd, go = tail(between, o, by_h, w, number, saved, bt=256 if saved else 512)
        terms = [(name, number, g) for name, g in zip(NAMES[4:] + NAMES[3:4], (gg, gu, gd, go))] + waiting
        dq, dk, dv, got, some = attend_back(q, k, v, do, lse, delta, terms, n, number)
        note(terms, got)
        squares.append(some)
        if number > 0:
            by_h, *weights = back(h, dh2, dq, dk, dv, tables, w, number)
            waiting = [(name, number, g) for name, g in zip(NAMES, weights)]
        else:
            got, total = finished(h, dq, dk, dv, tables, w, number, squares, n)
            note([(name, number) for name in NAMES[:3]], got)
    return sums, total


def solution(mesh):
    n = mesh.shape["dp"]

    def step(x, dy, *arrays):
        weights, m, v = (arrays[i : i + 7] for i in (0, 7, 14))
        sums, total = summed(x[0], dy[0], dict(zip(NAMES, weights)), n)
        new_w, new_m, new_v = stepped(sums, total, weights, m, v, n, sum(w.size for w in weights))
        whole = gathered(dict(zip(NAMES, new_w)), n)
        return (*whole, *new_m, *new_v)

    states, all_of, cut = P(("rep", "dp"), None, None), P(None, None, None), P(None, "dp", None)
    return jax.shard_map(
        step,
        mesh=mesh,
        in_specs=(states, states) + (all_of,) * 7 + (cut,) * 14,
        out_specs=(P("rep", None, None),) * 7 + (P("rep", "dp", None),) * 14,
        check_vma=False,
    )
```
